128 devices in a mesh: ice: 8 (over x, core), ocn: 16 (over z, y).
Axes of the slice: x: 4, y: 4, z: 4, core: 2. Of those that a mesh axis runs over, the one named last changes fastest.
Arguments:
- ice_state: bfloat16 [5, 20, 131072], P(None, None, ('ice', 'ocn')), may hold values from -6 to 6
- ocean_state: bfloat16 [5, 20, 131072], P(None, None, ('ice', 'ocn')), may hold values from -5 to 5
- ice_rate: float32 [5, 20], replicated, may hold values from 0.2 to 2
- block_weights: bfloat16 [16384, 128, 128], P(('ice', 'ocn')), may hold values from -0.1875 to 0.1875
- block_route: int32 [16384, 1], P(('ice', 'ocn')), may hold values from 0 to 127; in each aligned block of 128 rows (0 to 127, 128 to 255, ...) at most 2 rows name the same one
- block_tiles: int32 [16384, 2], P(('ice', 'ocn')), may hold values from 0 to 7
- block_valid: int32 [16384], P(('ice', 'ocn')), may hold values from 16 to 128
- ice_mask: int32 [131072], P(('ice', 'ocn')), may hold values 0 or 1
Outputs:
- ice_final: bfloat16 [5, 20, 131072], P(None, None, ('ice', 'ocn'))
- ocean_flux: bfloat16 [5, 20, 131072], P(None, None, ('ice', 'ocn'))
The draws below stay inside these ranges and needn't reach their ends.
Inputs may be any that keep to these rules, and one draw needn't show every extreme that they name: `block_route`: among the blocks of one device no destination appears more than 2 times.
All inputs are finite; a program needn't handle non-finite values. No bound on the sum of `ice_mask` on one device may be relied on, other than what follows from the above.
Results may differ from the reference program's by a relative error of at most 0.008.
Values may be sent and summed in bfloat16 or wider, within the bound.
A program may use at most 128 MiB of HBM per device.

```python
import math
import jax
import jax.numpy as jnp
import numpy as np
from jax import lax

CATS = 5
FIELDS = 20
BLOCK = 128
CAP = 2
TILES = 8
NB = 128
NI = 131072
NO = 131072
DEVICES = 128


def with_ends(values, stream_key, low, top_value):
    place = [jax.random.randint(jax.random.fold_in(stream_key, axis), (), 0, length) for axis, length in enumerate(values.shape)]
    widest = values.shape.index(max(values.shape))
    next_to = place[:widest] + [(place[widest] + 1) % values.shape[widest]] + place[widest + 1:]
    return values.at[tuple(place)].set(low).at[tuple(next_to)].set(top_value)


def levels(rng, extent, pieces, low, high):
    def one(position, shards_of):
        draws = jax.random.uniform(jax.random.fold_in(jax.random.fold_in(rng, 6), position), (shards_of,), jnp.float32, low / len(pieces), high / len(pieces))
        return jnp.repeat(jnp.exp(draws), extent[position] // shards_of).reshape((-1,) + (1,) * (len(extent) - position - 1))

    gain = one(*pieces[0])
    for cut in pieces[1:]:
        gain = gain * one(*cut)
    return gain


def routed_block(own_key, own, number, rows, count, top, reach, slope):
    ranking = jax.random.permutation(own_key, count)
    packed, ordinary = shares(count, rows * top, reach, slope, True), shares(count, rows * top, reach, slope, False)
    places = jnp.arange(count)

    def named(lengths, turn):
        used = int((lengths > 0).sum())
        fixed = max(1, used // 4)
        shifted = fixed + (places - fixed + turn * (used - fixed)) % max(1, count - fixed)
        return jnp.zeros((count,), jnp.int32).at[ranking[jnp.where(places < fixed, places, shifted)]].set(jnp.asarray(lengths, jnp.int32))

    lengths = jnp.where(number % 4 == 0, named(packed, number // 4), named(ordinary, number - number // 4 - 1))
    mixed = jax.random.permutation(jax.random.fold_in(own, 3), count)
    donor, receiver = mixed[0:count // 2 * 2:2], mixed[1:count // 2 * 2:2]
    slack = jnp.minimum(lengths[donor] - 1, reach - lengths[receiver]) // 2
    slack = jnp.where((donor == ranking[0]) | (receiver == ranking[0]) | (lengths[receiver] == 0), 0, jnp.maximum(slack, 0))
    shifted = jax.random.randint(jax.random.fold_in(own, 4), (count // 2,), 0, 1 << 20) % (slack + 1)
    lengths = lengths.at[donor].add(-shifted).at[receiver].add(shifted)
    members = jnp.searchsorted(jnp.cumsum(lengths), jnp.arange(rows * top), side="right").astype(jnp.int32)
    listing = members.reshape(top, rows).T
    listing = listing[jax.random.permutation(jax.random.fold_in(own, 1), rows)]
    turn = jax.random.randint(jax.random.fold_in(own, 2), (rows, 1), 0, top)
    return jnp.take_along_axis(listing, (jnp.arange(top)[None, :] + turn) % top, axis=1)


def shares(amount, total, limit, slope, full):
    weights = [(1 << 20) // math.isqrt(standing ** slope) + 1 for standing in range(1, amount + 1)]
    largest = limit if full else min(limit, max(-(-total // amount), total * weights[0] // sum(weights)))
    least = 1 if total - largest >= amount - 1 else 0
    holding, rest = [largest] + [least] * (amount - 1), total - largest - least * (amount - 1)
    while rest > 0:
        free = [i for i in range(1, amount) if holding[i] < largest] or [i for i in range(1, amount) if holding[i] < limit]
        whole, left = sum([weights[i] for i in free]), rest
        for i in free:
            addition = min(limit - holding[i], max(1, left * weights[i] // whole), rest)
            holding[i] = holding[i] + addition
            rest = rest - addition
    return np.array(holding)


def normal_values(own_key, shape, deviation, reach, pieces=(), held_as=jnp.bfloat16):
    array = deviation * jax.random.normal(own_key, shape, jnp.float32)
    if pieces:
        array = array * levels(own_key, shape, pieces, -0.22, 0.18)
    return jnp.clip(array, -reach, reach).astype(held_as)


def setup_inputs(seed: int = 0) -> dict:
    streams_of = jax.random.split(jax.random.key(seed), 9)
    ice_state = normal_values(streams_of[0], (CATS, FIELDS, NI), 1.0, 6.0, ((2, 128),))
    ocean_state = normal_values(streams_of[1], (CATS, FIELDS, NO), 0.7, 5.0, ((2, 128),))
    ice_rate = jnp.clip(jnp.exp(jax.random.uniform(streams_of[2], (CATS, FIELDS), jnp.float32, math.log(0.2), math.log(2.0))), 0.2, 2.0)
    block_weights = normal_values(streams_of[3], (NB * DEVICES, BLOCK, BLOCK), (NB * BLOCK // (2 * TILES)) ** -0.5, 0.1875, ((0, 128),))
    block_route_keys = jax.random.split(jax.random.fold_in(streams_of[4], 1), (NB * DEVICES) // NB)
    block_route_turns = jax.random.permutation(jax.random.fold_in(streams_of[4], 3), (NB * DEVICES) // NB)
    block_route = jax.vmap(lambda own, number: routed_block(jax.random.fold_in(streams_of[4], 2), own, number, NB, DEVICES, 1, CAP, 1))(block_route_keys, block_route_turns).reshape((NB * DEVICES, 1))
    block_tiles = with_ends(jax.random.randint(streams_of[5], (NB * DEVICES, 2), 0, TILES), jax.random.fold_in(streams_of[5], 1), 0, TILES - 1).astype(jnp.int32)
    block_valid = with_ends(jax.random.randint(streams_of[6], (NB * DEVICES,), BLOCK // 8, BLOCK + 1), jax.random.fold_in(streams_of[6], 1), BLOCK // 8, BLOCK).astype(jnp.int32)
    ice_mask = with_ends((jax.random.randint(streams_of[7], (NI,), 0, 4) < 3).astype(jnp.int32), jax.random.fold_in(streams_of[7], 1), 0, 1)
    return {"ice_state": ice_state, "ocean_state": ocean_state, "ice_rate": ice_rate, "block_weights": block_weights, "block_route": block_route, "block_tiles": block_tiles, "block_valid": block_valid, "ice_mask": ice_mask}


def reference(ice_state, ocean_state, ice_rate, block_weights, block_route, block_tiles, block_valid, ice_mask):
    chans = CATS * FIELDS
    live = jnp.arange(BLOCK, dtype=jnp.int32)[None, :] < block_valid[:, None]
    masked = jnp.where(live[:, :, None], block_weights, jnp.zeros((), jnp.bfloat16)).reshape(DEVICES, NB, BLOCK, BLOCK)
    route = block_route[:, 0].reshape(DEVICES, NB)
    source = block_tiles[:, 0].reshape(DEVICES, NB)
    target = (route * TILES + block_tiles[:, 1].reshape(DEVICES, NB)).astype(jnp.int32)
    rates = ice_rate.reshape(chans, 1).astype(jnp.float32)
    land = ice_mask.astype(jnp.float32)[None, :]
    ocean = ocean_state.reshape(chans, NO).astype(jnp.float32)
    ice = (ice_state * ice_mask.astype(jnp.bfloat16)[None, None, :]).reshape(chans, NI)
    flux = None
    for turn in range(2):
        tiles_all = jnp.transpose(ice.reshape(chans, DEVICES, TILES, BLOCK), (1, 0, 2, 3))

        def forward(acc, item):
            tile_set, weights, picks, places = item
            picked = tile_set[:, picks, :].astype(jnp.float32)
            prods = jnp.einsum("cbi,bio->bco", picked, weights.astype(jnp.float32)).astype(jnp.bfloat16)
            prods = lax.optimization_barrier(prods).astype(jnp.float32)
            return acc.at[places].add(prods), None

        start = jnp.zeros((DEVICES * TILES, chans, BLOCK), jnp.float32)
        ocean_in, unused = lax.scan(forward, start, (tiles_all, masked, source, target))
        ocean_in = jnp.transpose(ocean_in, (1, 0, 2)).reshape(chans, NO)
        flux = jnp.tanh(ocean_in + ocean).astype(jnp.bfloat16)
        flux_tiles = jnp.transpose(flux.reshape(chans, DEVICES * TILES, BLOCK), (1, 0, 2))

        def backward(carry, item):
            weights, picks, places = item
            taken = flux_tiles[places].astype(jnp.float32)
            contrib = jnp.einsum("bco,bio->bci", taken, weights.astype(jnp.float32))
            forced = jnp.zeros((TILES, chans, BLOCK), jnp.float32).at[picks].add(contrib)
            return carry, forced

        unused, forcing = lax.scan(backward, jnp.float32(0.0), (masked, source, target))
        forcing = jnp.transpose(forcing, (2, 0, 1, 3)).reshape(chans, NI)
        ice = (land * (ice.astype(jnp.float32) + rates * jnp.tanh(forcing))).astype(jnp.bfloat16)
    return ice.reshape(CATS, FIELDS, NI), flux.reshape(CATS, FIELDS, NO)
```

```python
import functools

import jax
import jax.numpy as jnp
from jax import lax
from jax.experimental import pallas as pl
from jax.experimental.pallas import tpu as pltpu
from jax.sharding import PartitionSpec as P

MESH = pl.DeviceIdType.MESH
F32 = jnp.float32
BF16 = jnp.bfloat16
I32 = jnp.int32

ROWS = (32, 32, 40)
BASE = (0, 32, 64)
CH = 104
NBLK = 128
TILES = 8
W = 128
DENSE = 128
ORDER = ((0, 1, 2), (1, 2, 0), (2, 0, 1))


def layout(cap):
    names = {}
    at = 0
    for part in range(3):
        for name, size in (
            ("perm", 8 * cap), ("keep", 8 * cap), ("last", DENSE),
            ("want", 8 * cap), ("blk", 8 * cap), ("slot", NBLK),
        ):
            names[name, part] = at
            at += size
    for name, size in (("src", NBLK), ("order", NBLK), ("same", NBLK), ("end", TILES), ("valid", NBLK)):
        names[name] = at
        at += size
    return names, at


def split(owner):
    ice, ocn = owner // 16, owner % 16
    return (ice // 2, ocn % 4, ocn // 4), ice % 2


def ranks(key):
    n = key.shape[0]
    where = jnp.arange(n, dtype=I32)
    before = (key[None, :] < key[:, None]) | ((key[None, :] == key[:, None]) & (where[None, :] < where[:, None]))
    rank = jnp.sum(before.astype(I32), axis=1)
    hit = rank[None, :] == where[:, None]
    perm = jnp.sum(jnp.where(hit, where[None, :], 0), axis=1)
    ordered = jnp.sum(jnp.where(hit, key[None, :], 0), axis=1)
    same = jnp.concatenate([jnp.zeros((1,), I32), (ordered[1:] == ordered[:-1]).astype(I32)])
    return perm, same


def ends(key, count, none):
    tile = jnp.arange(count, dtype=I32)
    upto = jnp.sum((key[None, :] <= tile[:, None]).astype(I32), axis=1) - 1
    any_ = jnp.sum((key[None, :] == tile[:, None]).astype(I32), axis=1) > 0
    return jnp.where(any_, upto, none)


def tables(cap, route, source, target, valid):
    me_ice, me_ocn = lax.axis_index("ice"), lax.axis_index("ocn")
    own = route * TILES + target
    every = lax.all_gather(own, ("ice", "ocn")).reshape(4, 2, 4, 4, NBLK)
    mine, my_core = split(me_ice * 16 + me_ocn)
    my_x, my_y, my_z = mine
    order = jnp.arange(NBLK, dtype=I32)
    pieces = []
    for part in range(3):
        first, second, third = ORDER[part]
        if part == 0:
            group = lax.dynamic_slice(every, (0, 0, my_z, my_y, 0), (4, 2, 1, 1, NBLK)).reshape(8, NBLK)
        elif part == 1:
            group = lax.dynamic_slice(every, (my_x, 0, my_z, 0, 0), (1, 2, 1, 4, NBLK)).reshape(2, 4, NBLK)
            group = jnp.transpose(group, (1, 0, 2)).reshape(8, NBLK)
        else:
            group = lax.dynamic_slice(every, (my_x, 0, 0, my_y, 0), (1, 2, 4, 1, NBLK)).reshape(2, 4, NBLK)
            group = jnp.transpose(group, (1, 0, 2)).reshape(8, NBLK)
        place, core = split(group // TILES)
        picked = (place[first] == mine[first]) & (core == my_core)
        dense = place[second] * 32 + place[third] * 8 + group % TILES
        earlier = order[None, :] < order[:, None]
        pos = jnp.sum((picked[:, None, :] & earlier[None]).astype(I32), axis=2)
        hit = picked[:, None, :] & (pos[:, None, :] == jnp.arange(cap, dtype=I32)[None, :, None])
        want = jnp.sum(jnp.where(hit, dense[:, None, :] + 1, 0), axis=2).reshape(8 * cap) - 1
        key = jnp.where(want < 0, 1000, want)
        perm, keep = ranks(key)
        last = ends(key, DENSE, 8 * cap)
        place, core = split(own // TILES)
        member = place[first] * 2 + core
        pos = jnp.sum(((member[None, :] == member[:, None]) & earlier).astype(I32), axis=1)
        slot = member * cap + pos
        hit = slot[None, :] == jnp.arange(8 * cap, dtype=I32)[:, None]
        blk = jnp.sum(jnp.where(hit, order[None, :], 0), axis=1)
        pieces += [perm, keep, last, jnp.maximum(want, 0), blk, slot]
    by_source, same = ranks(source)
    pieces += [source, by_source, same, ends(source, TILES, NBLK), valid]
    return jnp.concatenate(pieces)


def wait_in(ref, sem):
    pltpu.make_async_copy(ref, ref, sem).wait()


def body(cap, meta, ice_in, ocean, mask, rate, weights, ice_out, flux_out, ice_t, prod, pre, *rest):
    rest = list(rest)

    def take(count):
        out = rest[:count]
        del rest[:count]
        return out

    out_buf, in_buf, relay, back, back_relay = take(3), take(3), take(3), take(3), take(3)
    scan, dense, wide, rs1, rs2, rs3, rs4 = take(3), take(3), take(3), take(3), take(3), take(3), take(3)
    a_send, a_recv, r_send, r_recv, g_send, g_recv = rest
    names, unused = layout(cap)
    my_ice, my_ocn = lax.axis_index("ice"), lax.axis_index("ocn")
    x, core = my_ice // 2, my_ice % 2
    spot = (x, my_ocn % 4, my_ocn // 4)

    def device(axis, step, which):
        place = list(spot)
        place[axis] = (place[axis] + step + 4) % 4
        return (place[0] * 2 + which, place[2] * 4 + place[1])

    def push(src, dst, send, recv, to):
        copy = pltpu.make_async_remote_copy(src, dst, send, recv, device_id=to, device_id_type=MESH)
        copy.start()
        return copy

    barrier = pltpu.get_barrier_semaphore()
    peers = [(my_ice // 2 * 2 + 1 - core, my_ocn)]
    for axis in range(3):
        for step in (1, -1):
            peers += [device(axis, step, 0), device(axis, step, 1)]
    for peer in peers:
        pl.semaphore_signal(barrier, inc=1, device_id=peer, device_id_type=MESH)

    for tile in range(TILES):
        lanes = slice(tile * W, (tile + 1) * W)
        ice_t[tile] = (ice_in[:, lanes].astype(F32) * mask[:, lanes]).astype(BF16)
    for part in range(3):
        scan[part][8 * cap] = jnp.zeros((ROWS[part], W), BF16)
    pre[NBLK] = jnp.zeros((CH, W), F32)
    lane = lax.broadcasted_iota(I32, (CH, W), 1)
    pl.semaphore_wait(barrier, len(peers))

    def exchange(way, fill, into, hop):
        copies = []
        for part in range(3):
            axis = ORDER[part][0]
            q = spot[axis]
            for side, step in ((0, 1), (1, -1)):
                member = (q + 2) % 4 * 2 + side
                fill(part, member, out_buf[part], member)
                copies.append(push(
                    out_buf[part].at[pl.ds(member * cap, cap)], hop[part].at[side],
                    a_send.at[way, part, side], a_recv.at[way, part, 8 + side], device(axis, step, core)))
        for part in range(3):
            axis = ORDER[part][0]
            q = spot[axis]
            me = q * 2 + core
            for turn, (step, which) in enumerate(((1, 0), (-1, 0), (1, 1), (-1, 1))):
                member = (q + step + 4) % 4 * 2 + which
                fill(part, member, out_buf[part], member)
                copies.append(push(
                    out_buf[part].at[pl.ds(member * cap, cap)], into[part].at[pl.ds(me * cap, cap)],
                    a_send.at[way, part, 2 + turn], a_recv.at[way, part, me], device(axis, step, which)))
        for part in range(3):
            axis = ORDER[part][0]
            q = spot[axis]
            me = q * 2 + core
            member = q * 2 + 1 - core
            fill(part, member, out_buf[part], member)
            copies.append(push(
                out_buf[part].at[pl.ds(member * cap, cap)], into[part].at[pl.ds(me * cap, cap)],
                a_send.at[way, part, 6], a_recv.at[way, part, me], device(axis, 0, 1 - core)))
            fill(part, me, into[part], me)
        for part in range(3):
            axis = ORDER[part][0]
            q = spot[axis]
            for side, step in ((0, 1), (1, -1)):
                wait_in(hop[part].at[side], a_recv.at[way, part, 8 + side])
                origin = (q - step + 4) % 4 * 2 + core
                copies.append(push(
                    hop[part].at[side], into[part].at[pl.ds(origin * cap, cap)],
                    a_send.at[way, part, 7 + side], a_recv.at[way, part, origin], device(axis, step, side)))
        return copies

    def arrive(way, part, into):
        q = spot[ORDER[part][0]]
        for other in range(1, 8):
            member = (q * 2 + core + other) % 8
            wait_in(into[part].at[pl.ds(member * cap, cap)], a_recv.at[way, part, member])

    def scatter_start(part, level, ref, n, one, two):
        axis = ORDER[part][1 + level]
        q, half = spot[axis], n // 2
        send, recv = r_send.at[part, level], r_recv.at[part, level]
        far, up, down = (q + 2) % 4 * n, (q + 1) % 4 * n, (q + 3) % 4 * n
        there, here = device(axis, 1, core), device(axis, -1, core)
        return [
            push(ref.at[pl.ds(far, half)], one.at[0], send.at[0], recv.at[0], there),
            push(ref.at[pl.ds(far + half, half)], one.at[1], send.at[1], recv.at[1], here),
            push(ref.at[pl.ds(up + half, half)], two.at[0, pl.ds(half, half)], send.at[2], recv.at[2], there),
            push(ref.at[pl.ds(down, half)], two.at[1, pl.ds(0, half)], send.at[3], recv.at[3], here),
        ]

    def scatter_next(part, level, ref, n, one, two):
        axis = ORDER[part][1 + level]
        q, half = spot[axis], n // 2
        send, recv = r_send.at[part, level], r_recv.at[part, level]
        up, down = (q + 1) % 4 * n, (q + 3) % 4 * n
        there, here = device(axis, 1, core), device(axis, -1, core)
        wait_in(one.at[0], recv.at[0])
        near = pl.ds(up, half)
        ref[near] = (ref[near].astype(F32) + one[0].astype(F32)).astype(BF16)
        first = push(ref.at[near], two.at[0, pl.ds(0, half)], send.at[4], recv.at[4], there)
        wait_in(one.at[1], recv.at[1])
        near = pl.ds(down + half, half)
        ref[near] = (ref[near].astype(F32) + one[1].astype(F32)).astype(BF16)
        return [first, push(ref.at[near], two.at[1, pl.ds(half, half)], send.at[5], recv.at[5], here)]

    def scatter_end(part, level, ref, n, two):
        half = n // 2
        recv = r_recv.at[part, level]
        wait_in(two.at[0, pl.ds(half, half)], recv.at[2])
        wait_in(two.at[1, pl.ds(0, half)], recv.at[3])
        wait_in(two.at[0, pl.ds(0, half)], recv.at[4])
        wait_in(two.at[1, pl.ds(half, half)], recv.at[5])
        q = spot[ORDER[part][1 + level]]
        return ref[pl.ds(q * n, n)].astype(F32) + two[0].astype(F32) + two[1].astype(F32)

    def gather_start(part, level, n, at):
        axis = ORDER[part][1 + level]
        q, ref = spot[axis], wide[part]
        send, recv = g_send.at[part, level], g_recv.at[part, level]
        own = ref.at[pl.ds(at + q * n, n)]
        return [
            push(own, own, send.at[0], recv.at[0], device(axis, 1, core)),
            push(own, own, send.at[1], recv.at[1], device(axis, -1, core)),
        ]

    def gather_next(part, level, n, at):
        axis = ORDER[part][1 + level]
        q, ref, half = spot[axis], wide[part], n // 2
        send, recv = g_send.at[part, level], g_recv.at[part, level]
        low, high = at + (q + 3) % 4 * n, at + (q + 1) % 4 * n
        wait_in(ref.at[pl.ds(low, n)], recv.at[0])
        piece = ref.at[pl.ds(low, half)]
        first = push(piece, piece, send.at[2], recv.at[2], device(axis, 1, core))
        wait_in(ref.at[pl.ds(high, n)], recv.at[1])
        piece = ref.at[pl.ds(high + half, half)]
        return [first, push(piece, piece, send.at[3], recv.at[3], device(axis, -1, core))]

    def gather_end(part, level, n, at):
        q, ref, half = spot[ORDER[part][1 + level]], wide[part], n // 2
        recv = g_recv.at[part, level]
        far = at + (q + 2) % 4 * n
        wait_in(ref.at[pl.ds(far, half)], recv.at[2])
        wait_in(ref.at[pl.ds(far + half, half)], recv.at[3])

    def drain(copies):
        for copy in copies:
            copy.wait_send()

    def step(turn, carry):
        del turn

        def product(group, carry):
            for one in range(4):
                b = group * 4 + one
                tile = ice_t[meta[names["src"] + b]]
                tile = jnp.where(lane < meta[names["valid"] + b], tile, jnp.zeros((), BF16))
                prod[b] = jnp.dot(tile, weights[b], preferred_element_type=F32).astype(BF16)
            return carry

        lax.fori_loop(0, NBLK // 4, product, 0)

        def fill_products(part, member, ref, to):
            def put(k, carry):
                b = meta[names["blk", part] + member * cap + k]
                ref[to * cap + k] = prod[b, pl.ds(BASE[part], ROWS[part])]
                return carry

            lax.fori_loop(0, cap, put, 0, unroll=4)

        sent = exchange(0, fill_products, in_buf, relay)
        level0, level1 = [], []
        for part in range(3):
            arrive(0, part, in_buf)

            def add(group, acc, part=part):
                for one in range(4):
                    r = group * 4 + one
                    piece = in_buf[part][meta[names["perm", part] + r]].astype(F32)
                    acc = acc * meta[names["keep", part] + r].astype(F32) + piece
                    scan[part][r] = acc.astype(BF16)
                return acc

            lax.fori_loop(0, 2 * cap, add, jnp.zeros((ROWS[part], W), F32))

            def settle(t, carry, part=part):
                dense[part][t] = scan[part][meta[names["last", part] + t]]
                return carry

            lax.fori_loop(0, DENSE, settle, 0, unroll=8)
            level0 += scatter_start(part, 0, dense[part], 32, rs1[part], rs2[part])
        drain(sent)
        for part in range(3):
            level0 += scatter_next(part, 0, dense[part], 32, rs1[part], rs2[part])
        for part in range(3):
            q = spot[ORDER[part][1]]
            total = scatter_end(part, 0, dense[part], 32, rs2[part])
            dense[part][pl.ds(q * 32, 32)] = total.astype(BF16)
            level1 += scatter_start(part, 1, dense[part].at[pl.ds(q * 32, 32)], 8, rs3[part], rs4[part])
        for part in range(3):
            q = spot[ORDER[part][1]]
            level1 += scatter_next(part, 1, dense[part].at[pl.ds(q * 32, 32)], 8, rs3[part], rs4[part])
        drain(level0)
        gather1, gather0 = [], []
        for part in range(3):
            q, p = spot[ORDER[part][1]], spot[ORDER[part][2]]
            total = scatter_end(part, 1, dense[part].at[pl.ds(q * 32, 32)], 8, rs4[part])
            rows = slice(BASE[part], BASE[part] + ROWS[part])
            for tile in range(TILES):
                lanes = slice(tile * W, (tile + 1) * W)
                flux = jnp.tanh(total[tile] + ocean[rows, lanes].astype(F32)).astype(BF16)
                flux_out[rows, lanes] = flux
                wide[part][q * 32 + p * 8 + tile] = flux
            gather1 += gather_start(part, 1, 8, q * 32)
        drain(level1)
        for part in range(3):
            gather1 += gather_next(part, 1, 8, spot[ORDER[part][1]] * 32)
        for part in range(3):
            gather_end(part, 1, 8, spot[ORDER[part][1]] * 32)
            gather0 += gather_start(part, 0, 32, 0)
        drain(gather1)
        for part in range(3):
            gather0 += gather_next(part, 0, 32, 0)
        for part in range(3):
            gather_end(part, 0, 32, 0)
        drain(gather0)

        def fill_flux(part, member, ref, to):
            def put(k, carry):
                ref[to * cap + k] = wide[part][meta[names["want", part] + member * cap + k]]
                return carry

            lax.fori_loop(0, cap, put, 0, unroll=4)

        sent = exchange(1, fill_flux, back, back_relay)
        for part in range(3):
            arrive(1, part, back)

        def force(group, acc):
            for one in range(4):
                r = group * 4 + one
                b = meta[names["order"] + r]
                taken = jnp.concatenate([back[part][meta[names["slot", part] + b]] for part in range(3)], axis=0)
                term = lax.dot_general(taken, weights[b], (((1,), (1,)), ((), ())), preferred_element_type=F32)
                term = jnp.where(lane < meta[names["valid"] + b], term, 0.0)
                acc = acc * meta[names["same"] + r].astype(F32) + term
                pre[r] = acc
            return acc

        lax.fori_loop(0, NBLK // 4, force, jnp.zeros((CH, W), F32))
        for tile in range(TILES):
            lanes = slice(tile * W, (tile + 1) * W)
            forcing = pre[meta[names["end"] + tile]]
            new = (mask[:, lanes] * (ice_t[tile].astype(F32) + rate[...] * jnp.tanh(forcing))).astype(BF16)
            ice_t[tile] = new
            ice_out[:, lanes] = new
        drain(sent)
        return carry

    lax.fori_loop(0, 2, step, 0)


def couple(cap, meta, ice, ocean, mask, rate, weights):
    cells = TILES * W
    scratch = [pltpu.VMEM((TILES, CH, W), BF16), pltpu.VMEM((NBLK, CH, W), BF16), pltpu.VMEM((NBLK + 1, CH, W), F32)]
    for shape in (
        (8 * cap,), (8 * cap,), (2, cap), (8 * cap,), (2, cap), (8 * cap + 1,), (DENSE,), (DENSE,),
        (2, 16), (2, 32), (2, 4), (2, 8),
    ):
        scratch += [pltpu.VMEM(shape + (rows, W), BF16) for rows in ROWS]
    scratch += [
        pltpu.SemaphoreType.DMA((2, 3, 9)), pltpu.SemaphoreType.DMA((2, 3, 10)),
        pltpu.SemaphoreType.DMA((3, 2, 6)), pltpu.SemaphoreType.DMA((3, 2, 6)),
        pltpu.SemaphoreType.DMA((3, 2, 4)), pltpu.SemaphoreType.DMA((3, 2, 4)),
    ]
    vmem = pl.BlockSpec(memory_space=pltpu.VMEM)
    return pl.pallas_call(
        functools.partial(body, cap),
        out_shape=(jax.ShapeDtypeStruct((CH, cells), BF16), jax.ShapeDtypeStruct((CH, cells), BF16)),
        in_specs=[pl.BlockSpec(memory_space=pltpu.SMEM)] + [vmem] * 5,
        out_specs=(vmem, vmem),
        scratch_shapes=scratch,
        compiler_params=pltpu.CompilerParams(
            collective_id=0, has_side_effects=True, vmem_limit_bytes=66 * 1024 * 1024 - 2200000
        ),
    )(meta, ice, ocean, mask, rate, weights)


def on_device(ice_state, ocean_state, ice_rate, block_weights, block_route, block_tiles, block_valid, ice_mask):
    cats, fields, cells = ice_state.shape
    chans = cats * fields
    cap = 32
    meta = tables(cap, block_route[:, 0], block_tiles[:, 0], block_tiles[:, 1], block_valid)
    grow = ((0, CH - chans), (0, 0))
    ice = jnp.pad(ice_state.reshape(chans, cells), grow)
    ocean = jnp.pad(ocean_state.reshape(chans, cells), grow)
    rate = jnp.pad(ice_rate.reshape(chans, 1), grow)
    mask = ice_mask.astype(F32)[None, :]
    ice, flux = couple(cap, meta, ice, ocean, mask, rate, block_weights)
    return ice[:chans].reshape(cats, fields, cells), flux[:chans].reshape(cats, fields, cells)


def solution(mesh):
    placed = (
        P(None, None, ("ice", "ocn")),
        P(None, None, ("ice", "ocn")),
        P(),
        P(("ice", "ocn"), None, None),
        P(("ice", "ocn"), None),
        P(("ice", "ocn"), None),
        P(("ice", "ocn")),
        P(("ice", "ocn")),
    )
    return jax.shard_map(
        on_device,
        mesh=mesh,
        in_specs=placed,
        out_specs=(P(None, None, ("ice", "ocn")), P(None, None, ("ice", "ocn"))),
        check_vma=False,
    )
```

```python
import functools

import jax
import jax.numpy as jnp
from jax import lax
from jax.experimental import pallas as pl
from jax.experimental.pallas import tpu as pltpu
from jax.sharding import PartitionSpec as P

MESH = pl.DeviceIdType.MESH
F32 = jnp.float32
BF16 = jnp.bfloat16
I32 = jnp.int32

ROWS = (32, 32, 40)
BASE = (0, 32, 64)
CH = 104
NBLK = 128
TILES = 8
W = 128
MOST = 32
FEW = 20
DENSE = 128
ORDER = ((0, 1, 2), (1, 2, 0), (2, 0, 1))


def layout():
    names = {}
    at = 0
    for part in range(3):
        for name, size in (
            ("perm", 8 * MOST), ("keep", 8 * MOST), ("last", DENSE),
            ("want", 8 * MOST), ("blk", 8 * MOST), ("slot", NBLK),
        ):
            names[name, part] = at
            at += size
    for name, size in (("src", NBLK), ("order", NBLK), ("same", NBLK), ("end", TILES), ("valid", NBLK)):
        names[name] = at
        at += size
    return names, at


def split(owner):
    ice, ocn = owner // 16, owner % 16
    return (ice // 2, ocn % 4, ocn // 4), ice % 2


def ranks(key):
    n = key.shape[0]
    where = jnp.arange(n, dtype=I32)
    before = (key[None, :] < key[:, None]) | ((key[None, :] == key[:, None]) & (where[None, :] < where[:, None]))
    rank = jnp.sum(before.astype(I32), axis=1)
    hit = rank[None, :] == where[:, None]
    perm = jnp.sum(jnp.where(hit, where[None, :], 0), axis=1)
    ordered = jnp.sum(jnp.where(hit, key[None, :], 0), axis=1)
    same = jnp.concatenate([jnp.zeros((1,), I32), (ordered[1:] == ordered[:-1]).astype(I32)])
    return perm, same


def ends(key, count, none):
    tile = jnp.arange(count, dtype=I32)
    upto = jnp.sum((key[None, :] <= tile[:, None]).astype(I32), axis=1) - 1
    any_ = jnp.sum((key[None, :] == tile[:, None]).astype(I32), axis=1) > 0
    return jnp.where(any_, upto, none)


def tables(every, own, source, valid):
    me_ice, me_ocn = lax.axis_index("ice"), lax.axis_index("ocn")
    every = every.reshape(4, 4, 4, 2, NBLK)
    mine, my_core = split(me_ice * 16 + me_ocn)
    my_x, my_y, my_z = mine
    order = jnp.arange(NBLK, dtype=I32)
    pieces = []
    for part in range(3):
        first, second, third = ORDER[part]
        at, size = [my_z, my_y, my_x, 0, 0], [1, 1, 1, 2, NBLK]
        at[2 - first], size[2 - first] = 0, 4
        group = lax.dynamic_slice(every, at, size).reshape(8, NBLK)
        place, core = split(group // TILES)
        picked = (place[first] == mine[first]) & (core == my_core)
        dense = place[second] * 32 + place[third] * 8 + group % TILES
        earlier = order[None, :] < order[:, None]
        pos = jnp.sum((picked[:, None, :] & earlier[None]).astype(I32), axis=2)
        hit = picked[:, None, :] & (pos[:, None, :] == jnp.arange(MOST, dtype=I32)[None, :, None])
        want = jnp.sum(jnp.where(hit, dense[:, None, :] + 1, 0), axis=2).reshape(8 * MOST) - 1
        key = jnp.where(want < 0, 1000, want)
        perm, keep = ranks(key)
        last = ends(key, DENSE, 8 * MOST)
        place, core = split(own // TILES)
        member = place[first] * 2 + core
        pos = jnp.sum(((member[None, :] == member[:, None]) & earlier).astype(I32), axis=1)
        slot = member * MOST + pos
        hit = slot[None, :] == jnp.arange(8 * MOST, dtype=I32)[:, None]
        blk = jnp.sum(jnp.where(hit, order[None, :], 0), axis=1)
        pieces += [perm, keep, last, jnp.maximum(want, 0), blk, slot]
    by_source, same = ranks(source)
    pieces += [source, by_source, same, ends(source, TILES, NBLK), valid]
    return jnp.concatenate(pieces)


def most(every):
    place, core = split(every.reshape(NBLK, NBLK) // TILES)
    member = jnp.stack([place[axis] * 2 + core for axis in range(3)])
    hit = member[:, :, None, :] == jnp.arange(8, dtype=I32)[None, None, :, None]
    return jnp.max(jnp.sum(hit.astype(I32), axis=3))


def spread(own, every, send, recv):
    my_ice, my_ocn = lax.axis_index("ice"), lax.axis_index("ocn")
    y, z = my_ocn % 4, my_ocn // 4

    def near(k):
        return ((my_ice + k) % 8, my_ocn)

    def along_y(k):
        return (my_ice, z * 4 + (y + k) % 4)

    def along_z(k):
        return (my_ice, (z + k) % 4 * 4 + y)

    peers = [near(k) for k in range(1, 8)] + [along_y(k) for k in range(1, 4)] + [along_z(k) for k in range(1, 4)]
    barrier = pltpu.get_barrier_semaphore()
    for peer in peers:
        pl.semaphore_signal(barrier, inc=1, device_id=peer, device_id_type=MESH)
    line = my_ocn * 8
    every[line + my_ice] = own[...]
    pl.semaphore_wait(barrier, len(peers))

    def level(base, count, first, rows, to, mine):
        piece = every.at[pl.ds(first, rows)]
        copies = []
        for k in range(1, count):
            copies.append(pltpu.make_async_remote_copy(
                piece, piece, send.at[base + k], recv.at[base + mine], device_id=to(k), device_id_type=MESH))
            copies[-1].start()
        return copies

    def gathered(base, count, mine, where, rows):
        for k in range(1, count):
            other = (mine + k) % count
            wait_in(every.at[pl.ds(where(other), rows)], recv.at[base + other])

    sent = level(0, 8, line + my_ice, 1, near, my_ice)
    gathered(0, 8, my_ice, lambda k: line + k, 1)
    sent += level(8, 4, line, 8, along_y, y)
    gathered(8, 4, y, lambda k: (z * 4 + k) * 8, 8)
    sent += level(12, 4, z * 32, 32, along_z, z)
    gathered(12, 4, z, lambda k: k * 32, 32)
    for copy in sent:
        copy.wait_send()


def everyone(own):
    vmem = pl.BlockSpec(memory_space=pltpu.VMEM)
    return pl.pallas_call(
        spread,
        out_shape=jax.ShapeDtypeStruct((NBLK, 1, NBLK), I32),
        in_specs=[vmem],
        out_specs=vmem,
        scratch_shapes=[pltpu.SemaphoreType.DMA((16,)), pltpu.SemaphoreType.DMA((16,))],
        compiler_params=pltpu.CompilerParams(collective_id=0, has_side_effects=True),
    )(own.reshape(1, NBLK))


def wait_in(ref, sem):
    pltpu.make_async_copy(ref, ref, sem).wait()


def body(cap, meta, ice_in, ocean, mask, rate, weights, ice_out, flux_out, ice_t, prod, pre, *rest):
    rest = list(rest)

    def take(count):
        out = rest[:count]
        del rest[:count]
        return out

    out_buf, in_buf, relay, back, back_relay = take(3), take(3), take(3), take(3), take(3)
    scan, dense, wide, rs1, rs2, rs3, rs4 = take(3), take(3), take(3), take(3), take(3), take(3), take(3)
    a_send, a_recv, r_send, r_recv, g_send, g_recv = rest
    names, unused = layout()
    my_ice, my_ocn = lax.axis_index("ice"), lax.axis_index("ocn")
    x, core = my_ice // 2, my_ice % 2
    spot = (x, my_ocn % 4, my_ocn // 4)

    def device(axis, step, which):
        place = list(spot)
        place[axis] = (place[axis] + step + 4) % 4
        return (place[0] * 2 + which, place[2] * 4 + place[1])

    def push(src, dst, send, recv, to):
        copy = pltpu.make_async_remote_copy(src, dst, send, recv, device_id=to, device_id_type=MESH)
        copy.start()
        return copy

    barrier = pltpu.get_barrier_semaphore()
    peers = [(my_ice // 2 * 2 + 1 - core, my_ocn)]
    for axis in range(3):
        for step in (1, -1):
            peers += [device(axis, step, 0), device(axis, step, 1)]
    for peer in peers:
        pl.semaphore_signal(barrier, inc=1, device_id=peer, device_id_type=MESH)

    for tile in range(TILES):
        lanes = slice(tile * W, (tile + 1) * W)
        ice_t[tile] = (ice_in[:, lanes].astype(F32) * mask[:, lanes]).astype(BF16)
    for part in range(3):
        scan[part][8 * MOST] = jnp.zeros((ROWS[part], W), BF16)
    pre[NBLK] = jnp.zeros((CH, W), F32)
    lane = lax.broadcasted_iota(I32, (CH, W), 1)
    pl.semaphore_wait(barrier, len(peers))

    def exchange(way, fill, into, hop):
        copies = []
        for part in range(3):
            axis = ORDER[part][0]
            q = spot[axis]
            for side, step in ((0, 1), (1, -1)):
                member = (q + 2) % 4 * 2 + side
                fill(part, member, out_buf[part], member)
                copies.append(push(
                    out_buf[part].at[pl.ds(member * MOST, cap)], hop[part].at[side],
                    a_send.at[way, part, side], a_recv.at[way, part, 8 + side], device(axis, step, core)))
        for part in range(3):
            axis = ORDER[part][0]
            q = spot[axis]
            me = q * 2 + core
            for turn, (step, which) in enumerate(((1, 0), (-1, 0), (1, 1), (-1, 1))):
                member = (q + step + 4) % 4 * 2 + which
                fill(part, member, out_buf[part], member)
                copies.append(push(
                    out_buf[part].at[pl.ds(member * MOST, cap)], into[part].at[pl.ds(me * MOST, cap)],
                    a_send.at[way, part, 2 + turn], a_recv.at[way, part, me], device(axis, step, which)))
        for part in range(3):
            axis = ORDER[part][0]
            q = spot[axis]
            me = q * 2 + core
            member = q * 2 + 1 - core
            fill(part, member, out_buf[part], member)
            copies.append(push(
                out_buf[part].at[pl.ds(member * MOST, cap)], into[part].at[pl.ds(me * MOST, cap)],
                a_send.at[way, part, 6], a_recv.at[way, part, me], device(axis, 0, 1 - core)))
            fill(part, me, into[part], me)
        for part in range(3):
            axis = ORDER[part][0]
            q = spot[axis]
            for side, step in ((0, 1), (1, -1)):
                wait_in(hop[part].at[side], a_recv.at[way, part, 8 + side])
                origin = (q - step + 4) % 4 * 2 + core
                copies.append(push(
                    hop[part].at[side], into[part].at[pl.ds(origin * MOST, cap)],
                    a_send.at[way, part, 7 + side], a_recv.at[way, part, origin], device(axis, step, side)))
        return copies

    def arrive(way, part, into):
        q = spot[ORDER[part][0]]
        for other in range(1, 8):
            member = (q * 2 + core + other) % 8
            wait_in(into[part].at[pl.ds(member * MOST, cap)], a_recv.at[way, part, member])

    def scatter_start(part, level, ref, n, one, two):
        axis = ORDER[part][1 + level]
        q, half = spot[axis], n // 2
        send, recv = r_send.at[part, level], r_recv.at[part, level]
        far, up, down = (q + 2) % 4 * n, (q + 1) % 4 * n, (q + 3) % 4 * n
        there, here = device(axis, 1, core), device(axis, -1, core)
        return [
            push(ref.at[pl.ds(far, half)], one.at[0], send.at[0], recv.at[0], there),
            push(ref.at[pl.ds(far + half, half)], one.at[1], send.at[1], recv.at[1], here),
            push(ref.at[pl.ds(up + half, half)], two.at[0, pl.ds(half, half)], send.at[2], recv.at[2], there),
            push(ref.at[pl.ds(down, half)], two.at[1, pl.ds(0, half)], send.at[3], recv.at[3], here),
        ]

    def scatter_next(part, level, ref, n, one, two):
        axis = ORDER[part][1 + level]
        q, half = spot[axis], n // 2
        send, recv = r_send.at[part, level], r_recv.at[part, level]
        up, down = (q + 1) % 4 * n, (q + 3) % 4 * n
        there, here = device(axis, 1, core), device(axis, -1, core)
        wait_in(one.at[0], recv.at[0])
        near = pl.ds(up, half)
        ref[near] = (ref[near].astype(F32) + one[0].astype(F32)).astype(BF16)
        first = push(ref.at[near], two.at[0, pl.ds(0, half)], send.at[4], recv.at[4], there)
        wait_in(one.at[1], recv.at[1])
        near = pl.ds(down + half, half)
        ref[near] = (ref[near].astype(F32) + one[1].astype(F32)).astype(BF16)
        return [first, push(ref.at[near], two.at[1, pl.ds(half, half)], send.at[5], recv.at[5], here)]

    def scatter_end(part, level, ref, n, two):
        half = n // 2
        recv = r_recv.at[part, level]
        wait_in(two.at[0, pl.ds(half, half)], recv.at[2])
        wait_in(two.at[1, pl.ds(0, half)], recv.at[3])
        wait_in(two.at[0, pl.ds(0, half)], recv.at[4])
        wait_in(two.at[1, pl.ds(half, half)], recv.at[5])
        q = spot[ORDER[part][1 + level]]
        return ref[pl.ds(q * n, n)].astype(F32) + two[0].astype(F32) + two[1].astype(F32)

    def gather_start(part, level, n, at):
        axis = ORDER[part][1 + level]
        q, ref = spot[axis], wide[part]
        send, recv = g_send.at[part, level], g_recv.at[part, level]
        own = ref.at[pl.ds(at + q * n, n)]
        return [
            push(own, own, send.at[0], recv.at[0], device(axis, 1, core)),
            push(own, own, send.at[1], recv.at[1], device(axis, -1, core)),
        ]

    def gather_next(part, level, n, at):
        axis = ORDER[part][1 + level]
        q, ref, half = spot[axis], wide[part], n // 2
        send, recv = g_send.at[part, level], g_recv.at[part, level]
        low, high = at + (q + 3) % 4 * n, at + (q + 1) % 4 * n
        wait_in(ref.at[pl.ds(low, n)], recv.at[0])
        piece = ref.at[pl.ds(low, half)]
        first = push(piece, piece, send.at[2], recv.at[2], device(axis, 1, core))
        wait_in(ref.at[pl.ds(high, n)], recv.at[1])
        piece = ref.at[pl.ds(high + half, half)]
        return [first, push(piece, piece, send.at[3], recv.at[3], device(axis, -1, core))]

    def gather_end(part, level, n, at):
        q, ref, half = spot[ORDER[part][1 + level]], wide[part], n // 2
        recv = g_recv.at[part, level]
        far = at + (q + 2) % 4 * n
        wait_in(ref.at[pl.ds(far, half)], recv.at[2])
        wait_in(ref.at[pl.ds(far + half, half)], recv.at[3])

    def drain(copies):
        for copy in copies:
            copy.wait_send()

    def step(turn, carry):
        del turn

        def product(group, carry):
            for one in range(4):
                b = group * 4 + one
                tile = ice_t[meta[names["src"] + b]]
                tile = jnp.where(lane < meta[names["valid"] + b], tile, jnp.zeros((), BF16))
                prod[b] = jnp.dot(tile, weights[b], preferred_element_type=F32).astype(BF16)
            return carry

        lax.fori_loop(0, NBLK // 4, product, 0)

        def fill_products(part, member, ref, to):
            def put(k, carry):
                b = meta[names["blk", part] + member * MOST + k]
                ref[to * MOST + k] = prod[b, pl.ds(BASE[part], ROWS[part])]
                return carry

            lax.fori_loop(0, cap, put, 0, unroll=4)

        sent = exchange(0, fill_products, in_buf, relay)
        level0, level1 = [], []
        for part in range(3):
            arrive(0, part, in_buf)

            def add(group, acc, part=part):
                for one in range(4):
                    r = group * 4 + one
                    piece = in_buf[part][meta[names["perm", part] + r]].astype(F32)
                    acc = acc * meta[names["keep", part] + r].astype(F32) + piece
                    scan[part][r] = acc.astype(BF16)
                return acc

            lax.fori_loop(0, 2 * cap, add, jnp.zeros((ROWS[part], W), F32))

            def settle(t, carry, part=part):
                dense[part][t] = scan[part][meta[names["last", part] + t]]
                return carry

            lax.fori_loop(0, DENSE, settle, 0, unroll=8)
            level0 += scatter_start(part, 0, dense[part], 32, rs1[part], rs2[part])
        drain(sent)
        for part in range(3):
            level0 += scatter_next(part, 0, dense[part], 32, rs1[part], rs2[part])
        for part in range(3):
            q = spot[ORDER[part][1]]
            total = scatter_end(part, 0, dense[part], 32, rs2[part])
            dense[part][pl.ds(q * 32, 32)] = total.astype(BF16)
            level1 += scatter_start(part, 1, dense[part].at[pl.ds(q * 32, 32)], 8, rs3[part], rs4[part])
        for part in range(3):
            q = spot[ORDER[part][1]]
            level1 += scatter_next(part, 1, dense[part].at[pl.ds(q * 32, 32)], 8, rs3[part], rs4[part])
        drain(level0)
        gather1, gather0 = [], []
        for part in range(3):
            q, p = spot[ORDER[part][1]], spot[ORDER[part][2]]
            total = scatter_end(part, 1, dense[part].at[pl.ds(q * 32, 32)], 8, rs4[part])
            rows = slice(BASE[part], BASE[part] + ROWS[part])
            for tile in range(TILES):
                lanes = slice(tile * W, (tile + 1) * W)
                flux = jnp.tanh(total[tile] + ocean[rows, lanes].astype(F32)).astype(BF16)
                flux_out[rows, lanes] = flux
                wide[part][q * 32 + p * 8 + tile] = flux
            gather1 += gather_start(part, 1, 8, q * 32)
        drain(level1)
        for part in range(3):
            gather1 += gather_next(part, 1, 8, spot[ORDER[part][1]] * 32)
        for part in range(3):
            gather_end(part, 1, 8, spot[ORDER[part][1]] * 32)
            gather0 += gather_start(part, 0, 32, 0)
        drain(gather1)
        for part in range(3):
            gather0 += gather_next(part, 0, 32, 0)
        for part in range(3):
            gather_end(part, 0, 32, 0)
        drain(gather0)

        def fill_flux(part, member, ref, to):
            def put(k, carry):
                ref[to * MOST + k] = wide[part][meta[names["want", part] + member * MOST + k]]
                return carry

            lax.fori_loop(0, cap, put, 0, unroll=4)

        sent = exchange(1, fill_flux, back, back_relay)
        for part in range(3):
            arrive(1, part, back)

        def force(group, acc):
            for one in range(4):
                r = group * 4 + one
                b = meta[names["order"] + r]
                taken = jnp.concatenate([back[part][meta[names["slot", part] + b]] for part in range(3)], axis=0)
                term = lax.dot_general(taken, weights[b], (((1,), (1,)), ((), ())), preferred_element_type=F32)
                term = jnp.where(lane < meta[names["valid"] + b], term, 0.0)
                acc = acc * meta[names["same"] + r].astype(F32) + term
                pre[r] = acc
            return acc

        lax.fori_loop(0, NBLK // 4, force, jnp.zeros((CH, W), F32))
        for tile in range(TILES):
            lanes = slice(tile * W, (tile + 1) * W)
            forcing = pre[meta[names["end"] + tile]]
            new = (mask[:, lanes] * (ice_t[tile].astype(F32) + rate[...] * jnp.tanh(forcing))).astype(BF16)
            ice_t[tile] = new
            ice_out[:, lanes] = new
        drain(sent)
        return carry

    lax.fori_loop(0, 2, step, 0)


def couple(cap, which, meta, ice, ocean, mask, rate, weights):
    cells = TILES * W
    scratch = [pltpu.VMEM((TILES, CH, W), BF16), pltpu.VMEM((NBLK, CH, W), BF16), pltpu.VMEM((NBLK + 1, CH, W), F32)]
    for shape in (
        (8 * MOST,), (8 * MOST,), (2, cap), (8 * MOST,), (2, cap), (8 * MOST + 1,), (DENSE,), (DENSE,),
        (2, 16), (2, 32), (2, 4), (2, 8),
    ):
        scratch += [pltpu.VMEM(shape + (rows, W), BF16) for rows in ROWS]
    scratch += [
        pltpu.SemaphoreType.DMA((2, 3, 9)), pltpu.SemaphoreType.DMA((2, 3, 10)),
        pltpu.SemaphoreType.DMA((3, 2, 6)), pltpu.SemaphoreType.DMA((3, 2, 6)),
        pltpu.SemaphoreType.DMA((3, 2, 4)), pltpu.SemaphoreType.DMA((3, 2, 4)),
    ]
    vmem = pl.BlockSpec(memory_space=pltpu.VMEM)
    return pl.pallas_call(
        functools.partial(body, cap),
        out_shape=(jax.ShapeDtypeStruct((CH, cells), BF16), jax.ShapeDtypeStruct((CH, cells), BF16)),
        in_specs=[pl.BlockSpec(memory_space=pltpu.SMEM)] + [vmem] * 5,
        out_specs=(vmem, vmem),
        scratch_shapes=scratch,
        compiler_params=pltpu.CompilerParams(
            collective_id=which, has_side_effects=True, vmem_limit_bytes=66 * 1024 * 1024 - 2200000
        ),
    )(meta, ice, ocean, mask, rate, weights)


def on_device(ice_state, ocean_state, ice_rate, block_weights, block_route, block_tiles, block_valid, ice_mask):
    cats, fields, cells = ice_state.shape
    chans = cats * fields
    own = block_route[:, 0] * TILES + block_tiles[:, 1]
    every = everyone(own)
    meta = tables(every, own, block_tiles[:, 0], block_valid)
    grow = ((0, CH - chans), (0, 0))
    ice = jnp.pad(ice_state.reshape(chans, cells), grow)
    ocean = jnp.pad(ocean_state.reshape(chans, cells), grow)
    rate = jnp.pad(ice_rate.reshape(chans, 1), grow)
    mask = ice_mask.astype(F32)[None, :]
    ice, flux = lax.cond(
        most(every) <= FEW,
        functools.partial(couple, FEW, 1),
        functools.partial(couple, MOST, 2),
        meta, ice, ocean, mask, rate, block_weights,
    )
    return ice[:chans].reshape(cats, fields, cells), flux[:chans].reshape(cats, fields, cells)


def solution(mesh):
    placed = (
        P(None, None, ("ice", "ocn")),
        P(None, None, ("ice", "ocn")),
        P(),
        P(("ice", "ocn"), None, None),
        P(("ice", "ocn"), None),
        P(("ice", "ocn"), None),
        P(("ice", "ocn")),
        P(("ice", "ocn")),
    )
    return jax.shard_map(
        on_device,
        mesh=mesh,
        in_specs=placed,
        out_specs=(P(None, None, ("ice", "ocn")), P(None, None, ("ice", "ocn"))),
        check_vma=False,
    )
```

```python
import functools

import jax
import jax.numpy as jnp
from jax import lax
from jax.experimental import pallas as pl
from jax.experimental.pallas import tpu as pltpu
from jax.sharding import PartitionSpec as P

MESH = pl.DeviceIdType.MESH
F32 = jnp.float32
BF16 = jnp.bfloat16
I32 = jnp.int32

ROWS = (32, 32, 40)
HALVES = ((16, 16, 16), (16, 16, 24))
LEAD = 1
PLAN = (0,) * LEAD + (0, 1) * 40
LISTEN = 1
CH = 104
NBLK = 128
TILES = 8
W = 128
MOST = 32
FEW = 20
DENSE = 128
ORDER = ((0, 1, 2), (1, 2, 0), (2, 0, 1))


def split(owner):
    ice, ocn = owner >> 4, owner & 15
    return (ice >> 1, ocn & 3, ocn >> 2), ice & 1


def at_row(shape):
    return lax.broadcasted_iota(I32, shape, 0)


def at_lane(shape):
    return lax.broadcasted_iota(I32, shape, 1)


def down(values, keep):
    return jnp.sum(jnp.where(keep, values, 0), axis=0, keepdims=True)


def across(values, keep):
    return jnp.sum(jnp.where(keep, values, 0), axis=1, keepdims=True)


def column(row):
    n = row.shape[1]
    return across(row, at_row((n, n)) == at_lane((n, n)))


def line(col):
    n = col.shape[0]
    return down(col, at_row((n, n)) == at_lane((n, n)))


def sort_tables(key_row, key_col, count, none):
    n = key_row.shape[1]
    wide_row, wide_col = at_lane((n, n)), at_row((n, n))
    before = key_row * n + at_lane((1, n)) < key_col * n + at_row((n, 1))
    rank = across(1, before)
    hit = rank == wide_row
    perm = down(wide_col, hit)
    ordered = down(key_col, hit)
    earlier = down(key_col, rank + 1 == wide_row)
    same = jnp.where((ordered == earlier) & (at_lane((1, n)) > 0), 1, 0)
    tile = at_lane((n, W))
    upto = down(1, jnp.broadcast_to(key_col <= tile, (n, W))) - 1
    found = down(1, jnp.broadcast_to(key_col == tile, (n, W)))
    return perm, same, jnp.where(found > 0, upto, none)


def own_tables(goal, source):
    goal_col = column(goal)
    rows, most = [], jnp.zeros((1, NBLK), I32)
    earlier = at_row((NBLK, NBLK)) < at_lane((NBLK, NBLK))
    later = at_row((NBLK, NBLK)) > at_lane((NBLK, NBLK))
    blks = []
    for part in range(3):
        place, core = split(goal >> 3)
        member = place[ORDER[part][0]] * 2 + core
        place, core = split(goal_col >> 3)
        member_col = place[ORDER[part][0]] * 2 + core
        pos = down(1, (member_col == member) & earlier)
        pos_col = across(1, (member_col == member) & later)
        most = jnp.maximum(most, pos + 1)
        rows.append(member * MOST + pos)
        slot_col = member_col * MOST + pos_col
        for side in range(2):
            hit = slot_col == at_lane((NBLK, W)) + side * W
            blks.append(down(at_row((NBLK, W)), hit))
    order, same, end = sort_tables(source, column(source), TILES, NBLK)
    return rows + blks + [order, same, end], most


SLOT, BLK, BY_SOURCE, SAME, END, OWN_ROWS = 0, 3, 9, 10, 11, 16


def group_tables(part, goals, mine, my_core):
    first, second, third = ORDER[part]
    place, core = split(goals >> 3)
    picked = jnp.where((place[first] == mine[first]) & (core == my_core), 1, 0)
    dense = place[second] * 32 + place[third] * 8 + (goals & 7)
    pos = picked
    step = 1
    while step < NBLK:
        pos = pos + jnp.where(at_lane(pos.shape) >= step, pltpu.roll(pos, step, 1), 0)
        step *= 2
    pos = jnp.where(picked > 0, pos - 1, NBLK)
    k = at_row((MOST, NBLK))
    want = jnp.concatenate(
        [across(dense[m:m + 1] + 1, pos[m:m + 1] == k) for m in range(8)], axis=0) - 1
    key = jnp.where(want < 0, 1000, want)
    key_row = line(key)
    perm, keep, last = sort_tables(key_row, key, DENSE, 8 * MOST)
    want_row = jnp.where(key_row == 1000, 0, key_row)
    rows = []
    for one in (perm, keep, want_row):
        rows += [one[:, :W], one[:, W:]]
    return rows + [last]


PERM, KEEP, WANT, LAST, GROUP_ROWS = 0, 2, 4, 6, 24


def wait_in(ref, sem):
    pltpu.make_async_copy(ref, ref, sem).wait()


def body(cap, halves, unrolled, plan, src, valid, goal, source, ice_in, ocean, mask, rate, weights, ice_out, flux_out, over, *rest):
    rest = list(rest)

    def take(count):
        out = rest[:count]
        del rest[:count]
        return out

    count = len(halves)
    a_send, a_recv, r_send, r_recv, g_send, g_recv, m_send, m_recv, t_sem = rest[-9:]
    del rest[-9:]
    said, heard, own_v, group_v, own_s, group_s, vote_y, vote_z = rest[-8:]
    del rest[-8:]
    refs = [[take(1)[0] for unused in range(3)] + [take(3) for unused in range(12)] for half in range(count)]
    my_ice, my_ocn = lax.axis_index("ice"), lax.axis_index("ocn")
    x, core = my_ice // 2, my_ice % 2
    spot = (x, my_ocn % 4, my_ocn // 4)

    def device(axis, step, which):
        place = list(spot)
        place[axis] = (place[axis] + step + 4) % 4
        return (place[0] * 2 + which, place[2] * 4 + place[1])

    def push(src, dst, send, recv, to):
        copy = pltpu.make_async_remote_copy(src, dst, send, recv, device_id=to, device_id_type=MESH)
        copy.start()
        return copy

    def drain(copies):
        for copy in copies:
            copy.wait_send()
        copies.clear()

    def loop(size, unroll, one):
        def few(k, carry):
            one(k)
            return carry

        lax.fori_loop(0, size, few, 0, unroll=unroll)

    barrier = pltpu.get_barrier_semaphore()
    peers = [(my_ice // 2 * 2 + 1 - core, my_ocn)]
    for axis in range(3):
        for step in (1, -1):
            peers += [device(axis, step, 0), device(axis, step, 1)]
        peers += [device(axis, 2, 0), device(axis, 2, 1)]
    for peer in peers:
        pl.semaphore_signal(barrier, inc=1, device_id=peer, device_id_type=MESH)
    top = 0
    tops = []
    for half, rows in enumerate(halves):
        ice_t, prod, pre = refs[half][:3]
        tall = sum(rows)
        tops.append(top)
        for tile in range(TILES):
            lanes = slice(tile * W, (tile + 1) * W)
            ice_t[tile] = (ice_in[top:top + tall, lanes].astype(F32) * mask[:, lanes]).astype(BF16)
        for part in range(3):
            refs[half][8][part][8 * MOST] = jnp.zeros((rows[part], W), BF16)
        pre[NBLK] = jnp.zeros((tall, W), F32)
        top += tall
    tables, most = own_tables(goal[...], source[...])
    for row, one in enumerate(tables):
        own_v[row:row + 1] = one
    moved = pltpu.make_async_copy(own_v, own_s, t_sem.at[0])
    moved.start()
    said[0] = goal[...] + jnp.where(jnp.max(most, axis=1, keepdims=True) > cap, 1024, 0)
    for part in range(3):
        heard[part, spot[ORDER[part][0]] * 2 + core] = said[0]
    pl.semaphore_wait(barrier, len(peers))
    told = []
    for part in range(3):
        axis = ORDER[part][0]
        me = spot[axis] * 2 + core
        for turn, (step, flip) in enumerate(((0, 1), (1, 0), (1, 1), (2, 0), (2, 1), (3, 0), (3, 1))):
            other = 1 - core if flip else core
            told.append(push(
                said.at[0], heard.at[part, me], m_send.at[part, turn], m_recv.at[part, me], device(axis, step, other)))
    moved.wait()

    def listen():
        for part in range(3):
            me = spot[ORDER[part][0]] * 2 + core
            for other in range(1, 8):
                member = (me + other) % 8
                wait_in(heard.at[part, member], m_recv.at[part, member])
            goals = jnp.concatenate([heard[part, member] for member in range(8)], axis=0)
            if part == 0:
                vote_y[spot[1]] = jnp.max(goals >> 10, axis=0, keepdims=True)
                for step in range(1, 4):
                    told.append(push(
                        vote_y.at[spot[1]], vote_y.at[spot[1]], m_send.at[3, step], m_recv.at[3, spot[1]], device(1, step, core)))
            for row, one in enumerate(group_tables(part, goals & 1023, spot, core)):
                group_v[part * 7 + row:part * 7 + row + 1] = one
        copy = pltpu.make_async_copy(group_v, group_s, t_sem.at[1])
        copy.start()
        for step in range(1, 4):
            other = (spot[1] + step) % 4
            wait_in(vote_y.at[other], m_recv.at[3, other])
        vote_z[spot[2]] = jnp.maximum(jnp.maximum(vote_y[0], vote_y[1]), jnp.maximum(vote_y[2], vote_y[3]))
        for step in range(1, 4):
            told.append(push(
                vote_z.at[spot[2]], vote_z.at[spot[2]], m_send.at[4, step], m_recv.at[4, spot[2]], device(2, step, core)))
        copy.wait()

    def conclude():
        for step in range(1, 4):
            other = (spot[2] + step) % 4
            wait_in(vote_z.at[other], m_recv.at[4, other])
        over[...] = jnp.maximum(jnp.maximum(vote_z[0], vote_z[1]), jnp.maximum(vote_z[2], vote_z[3]))
        drain(told)

    def own_at(row, at):
        return own_s[row + (at >> 7), at & 127]

    def group_at(part, row, at):
        return group_s[part * 7 + row + (at >> 7), at & 127]

    def run(half, final):
        rows, top = halves[half], tops[half]
        tall = sum(rows)
        base = [sum(rows[:part]) for part in range(3)]
        ice_t, prod, pre, out_buf, in_buf, relay, back, back_relay, scan, dense, wide, rs1, rs2, rs3, rs4 = refs[half]
        lane = lax.broadcasted_iota(I32, (tall, W), 1)

        def exchange_start(way, fetch, into, hop):
            copies = []
            for part in range(3):
                q = spot[ORDER[part][0]]

                def fill(k, part=part, q=q):
                    for other in range(8):
                        member = (q * 2 + core + other) % 8
                        ref = out_buf if other else into
                        ref[part][member * MOST + k] = fetch(part, member * MOST + k)

                loop(cap, 1, fill)
                axis = ORDER[part][0]
                for side, step in ((0, 1), (1, -1)):
                    member = (q + 2) % 4 * 2 + side
                    copies.append(push(
                        out_buf[part].at[pl.ds(member * MOST, cap)], hop[part].at[side],
                        a_send.at[half, way, part, side], a_recv.at[half, way, part, 8 + side], device(axis, step, core)))
            for part in range(3):
                axis = ORDER[part][0]
                q = spot[axis]
                me = q * 2 + core
                for turn, (step, which) in enumerate(((1, 0), (-1, 0), (1, 1), (-1, 1), (0, 1 - core))):
                    member = (q + step + 4) % 4 * 2 + which
                    copies.append(push(
                        out_buf[part].at[pl.ds(member * MOST, cap)], into[part].at[pl.ds(me * MOST, cap)],
                        a_send.at[half, way, part, 2 + turn], a_recv.at[half, way, part, me], device(axis, step, which)))
            return copies

        def exchange_next(way, into, hop):
            copies = []
            for part in range(3):
                axis = ORDER[part][0]
                q = spot[axis]
                for side, step in ((0, 1), (1, -1)):
                    wait_in(hop[part].at[side], a_recv.at[half, way, part, 8 + side])
                    origin = (q - step + 4) % 4 * 2 + core
                    copies.append(push(
                        hop[part].at[side], into[part].at[pl.ds(origin * MOST, cap)],
                        a_send.at[half, way, part, 7 + side], a_recv.at[half, way, part, origin], device(axis, step, side)))
            return copies

        def arrive(way, into):
            for part in range(3):
                q = spot[ORDER[part][0]]
                for other in range(1, 8):
                    member = (q * 2 + core + other) % 8
                    wait_in(into[part].at[pl.ds(member * MOST, cap)], a_recv.at[half, way, part, member])

        def scatter_start(part, level, ref, at, n, one, two):
            axis = ORDER[part][1 + level]
            q, mid = spot[axis], n // 2
            send, recv = r_send.at[half, part, level], r_recv.at[half, part, level]
            far, up, down = at + (q + 2) % 4 * n, at + (q + 1) % 4 * n, at + (q + 3) % 4 * n
            there, here = device(axis, 1, core), device(axis, -1, core)
            return [
                push(ref.at[pl.ds(far, mid)], one.at[0], send.at[0], recv.at[0], there),
                push(ref.at[pl.ds(far + mid, mid)], one.at[1], send.at[1], recv.at[1], here),
                push(ref.at[pl.ds(up + mid, mid)], two.at[0, pl.ds(mid, mid)], send.at[2], recv.at[2], there),
                push(ref.at[pl.ds(down, mid)], two.at[1, pl.ds(0, mid)], send.at[3], recv.at[3], here),
            ]

        def scatter_next(part, level, ref, at, n, one, two):
            axis = ORDER[part][1 + level]
            q, mid = spot[axis], n // 2
            send, recv = r_send.at[half, part, level], r_recv.at[half, part, level]
            copies = []
            for side, step, to in ((0, 1, (q + 1) % 4 * n), (1, -1, (q + 3) % 4 * n + mid)):
                wait_in(one.at[side], recv.at[side])

                def join(k, side=side, to=to):
                    ref[at + to + k] = (ref[at + to + k].astype(F32) + one[side, k].astype(F32)).astype(BF16)

                loop(mid, 4, join)
                copies.append(push(
                    ref.at[pl.ds(at + to, mid)], two.at[side, pl.ds(side * mid, mid)],
                    send.at[4 + side], recv.at[4 + side], device(axis, step, core)))
            return copies

        def scatter_end(part, level, n, two):
            mid = n // 2
            recv = r_recv.at[half, part, level]
            wait_in(two.at[0, pl.ds(mid, mid)], recv.at[2])
            wait_in(two.at[1, pl.ds(0, mid)], recv.at[3])
            wait_in(two.at[0, pl.ds(0, mid)], recv.at[4])
            wait_in(two.at[1, pl.ds(mid, mid)], recv.at[5])

        def total(ref, at, two, k):
            return ref[at + k].astype(F32) + two[0, k].astype(F32) + two[1, k].astype(F32)

        def gather_start(part, level, n, at):
            axis = ORDER[part][1 + level]
            q, ref = spot[axis], wide[part]
            send, recv = g_send.at[half, part, level], g_recv.at[half, part, level]
            own = ref.at[pl.ds(at + q * n, n)]
            return [
                push(own, own, send.at[0], recv.at[0], device(axis, 1, core)),
                push(own, own, send.at[1], recv.at[1], device(axis, -1, core)),
            ]

        def gather_next(part, level, n, at):
            axis = ORDER[part][1 + level]
            q, ref, mid = spot[axis], wide[part], n // 2
            send, recv = g_send.at[half, part, level], g_recv.at[half, part, level]
            low, high = at + (q + 3) % 4 * n, at + (q + 1) % 4 * n
            wait_in(ref.at[pl.ds(low, n)], recv.at[0])
            piece = ref.at[pl.ds(low, mid)]
            first = push(piece, piece, send.at[2], recv.at[2], device(axis, 1, core))
            wait_in(ref.at[pl.ds(high, n)], recv.at[1])
            piece = ref.at[pl.ds(high + mid, mid)]
            return [first, push(piece, piece, send.at[3], recv.at[3], device(axis, -1, core))]

        def gather_end(part, level, n, at):
            q, ref, mid = spot[ORDER[part][1 + level]], wide[part], n // 2
            recv = g_recv.at[half, part, level]
            far = at + (q + 2) % 4 * n
            wait_in(ref.at[pl.ds(far, mid)], recv.at[2])
            wait_in(ref.at[pl.ds(far + mid, mid)], recv.at[3])

        def product(b):
            tile = ice_t[src[b]]
            tile = jnp.where(lane < valid[b], tile, jnp.zeros((), BF16))
            prod[b] = jnp.dot(tile, weights[b], preferred_element_type=F32).astype(BF16)

        def product_slot(part, at):
            return prod[own_at(BLK + 2 * part, at), pl.ds(base[part], rows[part])]

        def flux_slot(part, at):
            return wide[part][group_at(part, WANT, at)]

        parts = range(3)
        lines = [spot[ORDER[part][1]] * 32 for part in parts]
        loop(NBLK, 8, product)
        sent = exchange_start(0, product_slot, in_buf, relay)
        yield
        sent += exchange_next(0, in_buf, relay)
        yield
        arrive(0, in_buf)

        def add(group, accs):
            for one in range(4):
                r = group * 4 + one
                new = []
                for part in parts:
                    piece = in_buf[part][group_at(part, PERM, r)].astype(F32)
                    acc = accs[part] * group_at(part, KEEP, r).astype(F32) + piece
                    scan[part][r] = acc.astype(BF16)
                    new.append(acc)
                accs = tuple(new)
            return accs

        lax.fori_loop(0, 2 * cap, add, tuple(jnp.zeros((rows[part], W), F32) for part in parts))
        held = []
        for part in parts:
            def settle(t, part=part):
                dense[part][t] = scan[part][group_at(part, LAST, t)]

            loop(DENSE, 8, settle)
            held += scatter_start(part, 0, dense[part], 0, 32, rs1[part], rs2[part])
        yield
        for part in parts:
            held += scatter_next(part, 0, dense[part], 0, 32, rs1[part], rs2[part])
        yield
        for part in parts:
            scatter_end(part, 0, 32, rs2[part])

            def sum0(k, part=part):
                dense[part][lines[part] + k] = total(dense[part], lines[part], rs2[part], k).astype(BF16)

            loop(32, 4, sum0)
            held += scatter_start(part, 1, dense[part], lines[part], 8, rs3[part], rs4[part])
        yield
        for part in parts:
            held += scatter_next(part, 1, dense[part], lines[part], 8, rs3[part], rs4[part])
        drain(sent)
        yield
        spread_ = []
        for part in parts:
            scatter_end(part, 1, 8, rs4[part])
            at = lines[part] + spot[ORDER[part][2]] * 8
            here = slice(top + base[part], top + base[part] + rows[part])
            for tile in range(TILES):
                lanes = slice(tile * W, (tile + 1) * W)
                come = total(dense[part], at, rs4[part], tile)
                flux = jnp.tanh(come + ocean[here, lanes].astype(F32)).astype(BF16)
                if final:
                    flux_out[here, lanes] = flux
                wide[part][at + tile] = flux
            spread_ += gather_start(part, 1, 8, lines[part])
        yield
        for part in parts:
            spread_ += gather_next(part, 1, 8, lines[part])
        drain(held)
        yield
        for part in parts:
            gather_end(part, 1, 8, lines[part])
            spread_ += gather_start(part, 0, 32, 0)
        yield
        for part in parts:
            spread_ += gather_next(part, 0, 32, 0)
        yield
        for part in parts:
            gather_end(part, 0, 32, 0)
        sent = exchange_start(1, flux_slot, back, back_relay)
        yield
        sent += exchange_next(1, back, back_relay)
        drain(spread_)
        yield
        arrive(1, back)

        def force(group, acc):
            for one in range(4):
                r = group * 4 + one
                b = own_at(BY_SOURCE, r)
                taken = jnp.concatenate([back[part][own_at(SLOT + part, b)] for part in parts], axis=0)
                term = lax.dot_general(taken, weights[b], (((1,), (1,)), ((), ())), preferred_element_type=F32)
                term = jnp.where(lane < valid[b], term, 0.0)
                acc = acc * own_at(SAME, r).astype(F32) + term
                pre[r] = acc
            return acc

        lax.fori_loop(0, NBLK // 4, force, jnp.zeros((tall, W), F32))
        for tile in range(TILES):
            lanes = slice(tile * W, (tile + 1) * W)
            forcing = pre[own_at(END, tile)]
            change = rate[top:top + tall] * jnp.tanh(forcing)
            new = (mask[:, lanes] * (ice_t[tile].astype(F32) + change)).astype(BF16)
            ice_t[tile] = new
            if final:
                ice_out[top:top + tall, lanes] = new
        drain(sent)

    if not unrolled:
        listen()

        def whole(turn, carry):
            for half in range(count):
                for unused in run(half, True):
                    pass
            return carry

        lax.fori_loop(0, 2, whole, 0)
        conclude()
        return

    def both(half):
        yield from run(half, False)
        yield
        yield from run(half, True)

    live = [both(half) for half in range(count)]
    for at, half in enumerate(plan):
        next(live[half], None)
        if at == LISTEN:
            listen()
    for one in live:
        for unused in one:
            pass
    conclude()


def couple(cap, which, halves, unrolled, plan, src, valid, goal, source, ice, ocean, mask, rate, weights):
    cells = TILES * W
    scratch = []
    for rows in halves:
        tall = sum(rows)
        scratch += [pltpu.VMEM((TILES, tall, W), BF16), pltpu.VMEM((NBLK, tall, W), BF16), pltpu.VMEM((NBLK + 1, tall, W), F32)]
        for shape in (
            (8 * MOST,), (8 * MOST,), (2, cap), (8 * MOST,), (2, cap), (8 * MOST + 1,), (DENSE,), (DENSE,),
            (2, 16), (2, 32), (2, 4), (2, 8),
        ):
            scratch += [pltpu.VMEM(shape + (height, W), BF16) for height in rows]
    n = len(halves)
    scratch += [
        pltpu.VMEM((1, 1, NBLK), I32), pltpu.VMEM((3, 8, 1, NBLK), I32),
        pltpu.VMEM((OWN_ROWS, W), I32), pltpu.VMEM((GROUP_ROWS, W), I32),
        pltpu.SMEM((OWN_ROWS, W), I32), pltpu.SMEM((GROUP_ROWS, W), I32),
        pltpu.VMEM((4, 1, NBLK), I32), pltpu.VMEM((4, 1, NBLK), I32),
    ]
    scratch += [
        pltpu.SemaphoreType.DMA((n, 2, 3, 9)), pltpu.SemaphoreType.DMA((n, 2, 3, 10)),
        pltpu.SemaphoreType.DMA((n, 3, 2, 6)), pltpu.SemaphoreType.DMA((n, 3, 2, 6)),
        pltpu.SemaphoreType.DMA((n, 3, 2, 4)), pltpu.SemaphoreType.DMA((n, 3, 2, 4)),
        pltpu.SemaphoreType.DMA((5, 8)), pltpu.SemaphoreType.DMA((5, 8)), pltpu.SemaphoreType.DMA((2,)),
    ]
    vmem = pl.BlockSpec(memory_space=pltpu.VMEM)
    return pl.pallas_call(
        functools.partial(body, cap, halves, unrolled, plan),
        out_shape=(
            jax.ShapeDtypeStruct((CH, cells), BF16), jax.ShapeDtypeStruct((CH, cells), BF16), jax.ShapeDtypeStruct((1, NBLK), I32)
        ),
        in_specs=[pl.BlockSpec(memory_space=pltpu.SMEM)] * 2 + [vmem] * 7,
        out_specs=(vmem, vmem, vmem),
        scratch_shapes=scratch,
        compiler_params=pltpu.CompilerParams(
            collective_id=which, has_side_effects=True, vmem_limit_bytes=66 * 1024 * 1024 - 2200000
        ),
    )(src, valid, goal, source, ice, ocean, mask, rate, weights)


def on_device(ice_state, ocean_state, ice_rate, block_weights, block_route, block_tiles, block_valid, ice_mask):
    cats, fields, cells = ice_state.shape
    chans = cats * fields
    source = block_tiles[:, 0]
    goal = (block_route[:, 0] * TILES + block_tiles[:, 1]).reshape(1, NBLK)
    grow = ((0, CH - chans), (0, 0))
    ice = jnp.pad(ice_state.reshape(chans, cells), grow)
    ocean = jnp.pad(ocean_state.reshape(chans, cells), grow)
    rate = jnp.pad(ice_rate.reshape(chans, 1), grow)
    mask = ice_mask.astype(F32)[None, :]
    given = source, block_valid, goal, source.reshape(1, NBLK), ice, ocean, mask, rate, block_weights
    ice, flux, over = couple(FEW, 0, HALVES, True, PLAN, *given)

    def again(ice, flux, *given):
        ice, flux, unused = couple(MOST, 1, (ROWS,), False, (), *given)
        return ice, flux

    def keep(ice, flux, *given):
        return ice, flux

    ice, flux = lax.cond(jnp.max(over) > 0, again, keep, ice, flux, *given)
    return ice[:chans].reshape(cats, fields, cells), flux[:chans].reshape(cats, fields, cells)


def solution(mesh):
    placed = (
        P(None, None, ("ice", "ocn")),
        P(None, None, ("ice", "ocn")),
        P(),
        P(("ice", "ocn"), None, None),
        P(("ice", "ocn"), None),
        P(("ice", "ocn"), None),
        P(("ice", "ocn")),
        P(("ice", "ocn")),
    )
    return jax.shard_map(
        on_device,
        mesh=mesh,
        in_specs=placed,
        out_specs=(P(None, None, ("ice", "ocn")), P(None, None, ("ice", "ocn"))),
        check_vma=False,
    )
```

```python
import functools

import jax
import jax.numpy as jnp
from jax import lax
from jax.experimental import pallas as pl
from jax.experimental.pallas import tpu as pltpu
from jax.sharding import PartitionSpec as P

MESH = pl.DeviceIdType.MESH
F32 = jnp.float32
BF16 = jnp.bfloat16
I32 = jnp.int32

ROWS = (32, 32, 32, 4)
PARTS = len(ROWS)
TABLE = (0, 1, 2, 1)
HALVES = (ROWS,)
PLAN = tuple(int(one) for one in "0")
LISTEN = 0
CH = 100
NBLK = 128
TILES = 8
W = 128
MOST = 32
FEW = 20
DENSE = 128
ORDER = ((0, 1, 2), (1, 2, 0), (2, 0, 1), (1, 2, 0))


def split(owner):
    ice, ocn = owner >> 4, owner & 15
    return (ice >> 1, ocn & 3, ocn >> 2), ice & 1


def at_row(shape):
    return lax.broadcasted_iota(I32, shape, 0)


def at_lane(shape):
    return lax.broadcasted_iota(I32, shape, 1)


def down(values, keep):
    return jnp.sum(jnp.where(keep, values, 0), axis=0, keepdims=True)


def across(values, keep):
    return jnp.sum(jnp.where(keep, values, 0), axis=1, keepdims=True)


def column(row):
    n = row.shape[1]
    return across(row, at_row((n, n)) == at_lane((n, n)))


def line(col):
    n = col.shape[0]
    return down(col, at_row((n, n)) == at_lane((n, n)))


def sort_tables(key_row, key_col, count, none):
    n = key_row.shape[1]
    wide_row, wide_col = at_lane((n, n)), at_row((n, n))
    before = key_row * n + at_lane((1, n)) < key_col * n + at_row((n, 1))
    rank = across(1, before)
    hit = rank == wide_row
    perm = down(wide_col, hit)
    ordered = down(key_col, hit)
    earlier = down(key_col, rank + 1 == wide_row)
    same = jnp.where((ordered == earlier) & (at_lane((1, n)) > 0), 1, 0)
    tile = at_lane((n, W))
    upto = down(1, jnp.broadcast_to(key_col <= tile, (n, W))) - 1
    found = down(1, jnp.broadcast_to(key_col == tile, (n, W)))
    return perm, same, jnp.where(found > 0, upto, none)


def own_tables(goal, source):
    goal_col = column(goal)
    rows, most = [], jnp.zeros((1, NBLK), I32)
    earlier = at_row((NBLK, NBLK)) < at_lane((NBLK, NBLK))
    later = at_row((NBLK, NBLK)) > at_lane((NBLK, NBLK))
    blks = []
    for part in range(3):
        place, core = split(goal >> 3)
        member = place[ORDER[part][0]] * 2 + core
        place, core = split(goal_col >> 3)
        member_col = place[ORDER[part][0]] * 2 + core
        pos = down(1, (member_col == member) & earlier)
        pos_col = across(1, (member_col == member) & later)
        most = jnp.maximum(most, pos + 1)
        rows.append(member * MOST + pos)
        slot_col = member_col * MOST + pos_col
        for side in range(2):
            hit = slot_col == at_lane((NBLK, W)) + side * W
            blks.append(down(at_row((NBLK, W)), hit))
    order, same, end = sort_tables(source, column(source), TILES, NBLK)
    return rows + blks + [order, same, end], most


SLOT, BLK, BY_SOURCE, SAME, END, OWN_ROWS = 0, 3, 9, 10, 11, 16


def group_tables(part, goals, mine, my_core):
    first, second, third = ORDER[part]
    place, core = split(goals >> 3)
    picked = jnp.where((place[first] == mine[first]) & (core == my_core), 1, 0)
    dense = place[second] * 32 + place[third] * 8 + (goals & 7)
    pos = picked
    step = 1
    while step < NBLK:
        pos = pos + jnp.where(at_lane(pos.shape) >= step, pltpu.roll(pos, step, 1), 0)
        step *= 2
    pos = jnp.where(picked > 0, pos - 1, NBLK)
    k = at_row((MOST, NBLK))
    want = jnp.concatenate(
        [across(dense[m:m + 1] + 1, pos[m:m + 1] == k) for m in range(8)], axis=0) - 1
    key = jnp.where(want < 0, 1000, want)
    key_row = line(key)
    perm, keep, last = sort_tables(key_row, key, DENSE, 8 * MOST)
    want_row = jnp.where(key_row == 1000, 0, key_row)
    rows = []
    for one in (perm, keep, want_row):
        rows += [one[:, :W], one[:, W:]]
    return rows + [last]


PERM, KEEP, WANT, LAST, GROUP_ROWS = 0, 2, 4, 6, 24


def wait_in(ref, sem):
    pltpu.make_async_copy(ref, ref, sem).wait()


def body(cap, halves, unrolled, plan, src, valid, goal, source, ice_in, ocean, mask, rate, blocks, ice_out, flux_out, over, *rest):
    rest = list(rest)

    def take(count):
        out = rest[:count]
        del rest[:count]
        return out

    count = len(halves)
    a_send, a_recv, r_send, r_recv, g_send, g_recv, m_send, m_recv, t_sem = rest[-9:]
    del rest[-9:]
    said, heard, own_v, group_v, own_s, group_s, vote_y, vote_z, weights, turned = rest[-10:]
    del rest[-10:]
    loading = pltpu.make_async_copy(blocks, weights, t_sem.at[2])
    loading.start()
    refs = [[take(1)[0] for unused in range(3)] + [take(PARTS) for unused in range(12)] for half in range(count)]
    my_ice, my_ocn = lax.axis_index("ice"), lax.axis_index("ocn")
    x, core = my_ice // 2, my_ice % 2
    spot = (x, my_ocn % 4, my_ocn // 4)

    def device(axis, step, which):
        place = list(spot)
        place[axis] = (place[axis] + step + 4) % 4
        return (place[0] * 2 + which, place[2] * 4 + place[1])

    def push(src, dst, send, recv, to):
        copy = pltpu.make_async_remote_copy(src, dst, send, recv, device_id=to, device_id_type=MESH)
        copy.start()
        return copy

    def drain(copies):
        for copy in copies:
            copy.wait_send()
        copies.clear()

    def loop(size, unroll, one):
        def few(k, carry):
            one(k)
            return carry

        lax.fori_loop(0, size, few, 0, unroll=unroll)

    barrier = pltpu.get_barrier_semaphore()
    peers = [(my_ice // 2 * 2 + 1 - core, my_ocn)]
    for axis in range(3):
        for step in (1, -1):
            peers += [device(axis, step, 0), device(axis, step, 1)]
        peers += [device(axis, 2, 0), device(axis, 2, 1)]
    for peer in peers:
        pl.semaphore_signal(barrier, inc=1, device_id=peer, device_id_type=MESH)
    top = 0
    tops = []
    for half, rows in enumerate(halves):
        ice_t, prod, pre = refs[half][:3]
        tall = sum(rows)
        tops.append(top)
        for tile in range(TILES):
            lanes = slice(tile * W, (tile + 1) * W)
            ice_t[tile] = (ice_in[top:top + tall, lanes].astype(F32) * mask[:, lanes]).astype(BF16)
        for part in range(PARTS):
            refs[half][8][part][8 * MOST] = jnp.zeros((rows[part], W), BF16)
        pre[NBLK] = jnp.zeros((tall, W), F32)
        top += tall
    tables, most = own_tables(goal[...], source[...])
    for row, one in enumerate(tables):
        own_v[row:row + 1] = one
    moved = pltpu.make_async_copy(own_v, own_s, t_sem.at[0])
    moved.start()
    said[0] = goal[...] + jnp.where(jnp.max(most, axis=1, keepdims=True) > cap, 1024, 0)
    for part in range(3):
        heard[part, spot[ORDER[part][0]] * 2 + core] = said[0]
    pl.semaphore_wait(barrier, len(peers))
    told = []
    for part in range(3):
        axis = ORDER[part][0]
        me = spot[axis] * 2 + core
        for turn, (step, flip) in enumerate(((0, 1), (1, 0), (1, 1), (2, 0), (2, 1), (3, 0), (3, 1))):
            other = 1 - core if flip else core
            told.append(push(
                said.at[0], heard.at[part, me], m_send.at[part, turn], m_recv.at[part, me], device(axis, step, other)))
    loading.wait()
    if not unrolled:
        moved.wait()

    def listen():
        for part in range(3):
            me = spot[ORDER[part][0]] * 2 + core
            for other in range(1, 8):
                member = (me + other) % 8
                wait_in(heard.at[part, member], m_recv.at[part, member])
            goals = jnp.concatenate([heard[part, member] for member in range(8)], axis=0)
            if part == 0:
                vote_y[spot[1]] = jnp.max(goals >> 10, axis=0, keepdims=True)
                for step in range(1, 4):
                    told.append(push(
                        vote_y.at[spot[1]], vote_y.at[spot[1]], m_send.at[3, step], m_recv.at[3, spot[1]], device(1, step, core)))
            for row, one in enumerate(group_tables(part, goals & 1023, spot, core)):
                group_v[part * 7 + row:part * 7 + row + 1] = one
        copy = pltpu.make_async_copy(group_v, group_s, t_sem.at[1])
        copy.start()
        for step in range(1, 4):
            other = (spot[1] + step) % 4
            wait_in(vote_y.at[other], m_recv.at[3, other])
        vote_z[spot[2]] = jnp.maximum(jnp.maximum(vote_y[0], vote_y[1]), jnp.maximum(vote_y[2], vote_y[3]))
        for step in range(1, 4):
            told.append(push(
                vote_z.at[spot[2]], vote_z.at[spot[2]], m_send.at[4, step], m_recv.at[4, spot[2]], device(2, step, core)))
        copy.wait()

        def turn_round(b):
            turned[b] = weights[b].T

        loop(NBLK, 4, turn_round)

    def conclude():
        for step in range(1, 4):
            other = (spot[2] + step) % 4
            wait_in(vote_z.at[other], m_recv.at[4, other])
        over[0] = jnp.max(jnp.maximum(jnp.maximum(vote_z[0], vote_z[1]), jnp.maximum(vote_z[2], vote_z[3])))
        drain(told)

    def run(half, final):
        rows, top = halves[half], tops[half]
        tall = sum(rows)
        base = [sum(rows[:part]) for part in range(PARTS)]
        ice_t, prod, pre, out_buf, in_buf, relay, back, back_relay, scan, dense, wide, rs1, rs2, rs3, rs4 = refs[half]
        lane = lax.broadcasted_iota(I32, (tall, W), 1)

        def exchange_start(way, fetch, into, hop):
            copies = []
            for part in range(PARTS):
                q = spot[ORDER[part][0]]

                members = [(q * 2 + core + other) % 8 for other in range(8)]
                lines_of = [(member // 4, member % 4 * MOST, member * MOST) for member in members]

                def fill(k, part=part, lines_of=lines_of):
                    got = [fetch(part, row, at + k) for row, at, unused in lines_of]
                    for other in range(8):
                        ref = out_buf if other else into
                        ref[part][lines_of[other][2] + k] = got[other]

                loop(cap, 2, fill)
                axis = ORDER[part][0]
                for side, step in ((0, 1), (1, -1)):
                    member = (q + 2) % 4 * 2 + side
                    copies.append(push(
                        out_buf[part].at[pl.ds(member * MOST, cap)], hop[part].at[side],
                        a_send.at[half, way, part, side], a_recv.at[half, way, part, 8 + side], device(axis, step, core)))
            for part in range(PARTS):
                axis = ORDER[part][0]
                q = spot[axis]
                me = q * 2 + core
                for turn, (step, which) in enumerate(((1, 0), (-1, 0), (1, 1), (-1, 1), (0, 1 - core))):
                    member = (q + step + 4) % 4 * 2 + which
                    copies.append(push(
                        out_buf[part].at[pl.ds(member * MOST, cap)], into[part].at[pl.ds(me * MOST, cap)],
                        a_send.at[half, way, part, 2 + turn], a_recv.at[half, way, part, me], device(axis, step, which)))
            return copies

        def exchange_next(way, into, hop):
            copies = []
            for part in range(PARTS):
                axis = ORDER[part][0]
                q = spot[axis]
                for side, step in ((0, 1), (1, -1)):
                    wait_in(hop[part].at[side], a_recv.at[half, way, part, 8 + side])
                    origin = (q - step + 4) % 4 * 2 + core
                    copies.append(push(
                        hop[part].at[side], into[part].at[pl.ds(origin * MOST, cap)],
                        a_send.at[half, way, part, 7 + side], a_recv.at[half, way, part, origin], device(axis, step, side)))
            return copies

        def arrive(way, part, into):
            q = spot[ORDER[part][0]]
            for other in range(1, 8):
                member = (q * 2 + core + other) % 8
                wait_in(into[part].at[pl.ds(member * MOST, cap)], a_recv.at[half, way, part, member])

        def scatter_far(part, key, axis, ref, at, stride, one, n):
            q, mid = spot[axis], n // 2
            far = at + (q + 2) % 4 * stride
            send, recv = r_send.at[half, part, key], r_recv.at[half, part, key]
            return [
                push(ref.at[pl.ds(far, mid)], one.at[0], send.at[0], recv.at[0], device(axis, 1, core)),
                push(ref.at[pl.ds(far + mid, mid)], one.at[1], send.at[1], recv.at[1], device(axis, -1, core)),
            ]

        def scatter_near(part, key, axis, ref, at, stride, two, n):
            q, mid = spot[axis], n // 2
            up, below = at + (q + 1) % 4 * stride, at + (q + 3) % 4 * stride
            send, recv = r_send.at[half, part, key], r_recv.at[half, part, key]
            return [
                push(ref.at[pl.ds(up + mid, mid)], two.at[0, pl.ds(mid, mid)], send.at[2], recv.at[2], device(axis, 1, core)),
                push(ref.at[pl.ds(below, mid)], two.at[1, pl.ds(0, mid)], send.at[3], recv.at[3], device(axis, -1, core)),
            ]

        def scatter_next(part, key, axis, ref, at, stride, one, two, n):
            q, mid = spot[axis], n // 2
            send, recv = r_send.at[half, part, key], r_recv.at[half, part, key]
            copies = []
            for side, step, to in ((0, 1, at + (q + 1) % 4 * stride), (1, -1, at + (q + 3) % 4 * stride + mid)):
                wait_in(one.at[side], recv.at[side])
                for k in range(mid):
                    ref[to + k] = (ref[to + k].astype(F32) + one[side, k].astype(F32)).astype(BF16)
                copies.append(push(
                    ref.at[pl.ds(to, mid)], two.at[side, pl.ds(side * mid, mid)],
                    send.at[4 + side], recv.at[4 + side], device(axis, step, core)))
            return copies

        def scatter_end(part, key, two, n):
            mid = n // 2
            recv = r_recv.at[half, part, key]
            wait_in(two.at[0, pl.ds(mid, mid)], recv.at[2])
            wait_in(two.at[1, pl.ds(0, mid)], recv.at[3])
            wait_in(two.at[0, pl.ds(0, mid)], recv.at[4])
            wait_in(two.at[1, pl.ds(mid, mid)], recv.at[5])

        def total(ref, at, two, k):
            return ref[at + k].astype(F32) + two[0, k].astype(F32) + two[1, k].astype(F32)

        def gather_start(part, key, axis, at, stride):
            q, ref = spot[axis], wide[part]
            send, recv = g_send.at[half, part, key], g_recv.at[half, part, key]
            own = ref.at[pl.ds(at + q * stride, 8)]
            return [
                push(own, own, send.at[0], recv.at[0], device(axis, 1, core)),
                push(own, own, send.at[1], recv.at[1], device(axis, -1, core)),
            ]

        def gather_next(part, key, axis, at, stride):
            q, ref = spot[axis], wide[part]
            send, recv = g_send.at[half, part, key], g_recv.at[half, part, key]
            low, high = at + (q + 3) % 4 * stride, at + (q + 1) % 4 * stride
            wait_in(ref.at[pl.ds(low, 8)], recv.at[0])
            piece = ref.at[pl.ds(low, 4)]
            first = push(piece, piece, send.at[2], recv.at[2], device(axis, 1, core))
            wait_in(ref.at[pl.ds(high, 8)], recv.at[1])
            piece = ref.at[pl.ds(high + 4, 4)]
            return [first, push(piece, piece, send.at[3], recv.at[3], device(axis, -1, core))]

        def gather_end(part, key, axis, at, stride):
            q, ref = spot[axis], wide[part]
            recv = g_recv.at[half, part, key]
            far = at + (q + 2) % 4 * stride
            wait_in(ref.at[pl.ds(far, 4)], recv.at[2])
            wait_in(ref.at[pl.ds(far + 4, 4)], recv.at[3])

        def product(b):
            tile = ice_t[src[b]]
            tile = jnp.where(lane < valid[b], tile, jnp.zeros((), BF16))
            prod[b] = jnp.dot(tile, weights[b], preferred_element_type=F32).astype(BF16)

        def product_slot(part, row, at):
            return prod[own_s[BLK + 2 * TABLE[part] + row, at], pl.ds(base[part], rows[part])]

        def flux_slot(part, row, at):
            return wide[part][group_s[7 * TABLE[part] + WANT + row, at]]

        parts = range(PARTS)
        second, third = [ORDER[part][1] for part in parts], [ORDER[part][2] for part in parts]
        lines = [spot[second[part]] * 32 for part in parts]
        loop(NBLK, 8, product)
        if unrolled and not final and half == 0:
            moved.wait()
        sent = exchange_start(0, product_slot, in_buf, relay)
        yield
        sent += exchange_next(0, in_buf, relay)
        yield
        held = []
        for part in parts:
            arrive(0, part, in_buf)
            acc = jnp.zeros((rows[part], W), F32)
            for line_, steps in ((0, min(W, 8 * cap)), (1, 8 * cap - W)):
                def add(group, acc, part=part, line_=line_):
                    for one in range(8):
                        r = group * 8 + one
                        piece = in_buf[part][group_s[7 * TABLE[part] + PERM + line_, r]].astype(F32)
                        acc = acc * group_s[7 * TABLE[part] + KEEP + line_, r].astype(F32) + piece
                        scan[part][line_ * W + r] = acc.astype(BF16)
                    return acc

                acc = lax.fori_loop(0, steps // 8, add, acc)
            for d in (2, 1, 3, 0):
                at = (spot[third[part]] + d) % 4 * 8

                def settle(k, part=part, at=at):
                    got = [scan[part][group_s[7 * TABLE[part] + LAST, k * 32 + at + tile]] for tile in range(8)]
                    for tile in range(8):
                        dense[part][k * 32 + at + tile] = got[tile]

                loop(4, 1, settle)
                held += scatter_far(part, 1 + d, second[part], dense[part], at, 32, rs1[part].at[d], 8)
                held += scatter_near(part, 1 + d, second[part], dense[part], at, 32, rs2[part].at[d], 8)
        yield
        for d in (2, 1, 3, 0):
            for part in parts:
                at = (spot[third[part]] + d) % 4 * 8
                held += scatter_next(part, 1 + d, second[part], dense[part], at, 32, rs1[part].at[d], rs2[part].at[d], 8)
        yield

        def collect(part, d):
            scatter_end(part, 1 + d, rs2[part].at[d], 8)
            at = lines[part] + (spot[third[part]] + d) % 4 * 8
            for k in range(8):
                dense[part][at + k] = total(dense[part], at, rs2[part].at[d], k).astype(BF16)

        for part in parts:
            collect(part, 2)
            held += scatter_far(part, 0, third[part], dense[part], lines[part], 8, rs3[part], 8)
        for part in parts:
            collect(part, 1)
            collect(part, 3)
            held += scatter_near(part, 0, third[part], dense[part], lines[part], 8, rs4[part], 8)
        yield
        for part in parts:
            held += scatter_next(part, 0, third[part], dense[part], lines[part], 8, rs3[part], rs4[part], 8)
        for part in parts:
            collect(part, 0)
        drain(sent)
        yield
        spread_ = []
        for part in parts:
            scatter_end(part, 0, rs4[part], 8)
            at = lines[part] + spot[third[part]] * 8
            here = slice(top + base[part], top + base[part] + rows[part])
            for tile in range(TILES):
                lanes = slice(tile * W, (tile + 1) * W)
                come = total(dense[part], at, rs4[part], tile)
                flux = jnp.tanh(come + ocean[here, lanes].astype(F32)).astype(BF16)
                if final:
                    flux_out[here, lanes] = flux
                wide[part][at + tile] = flux
            spread_ += gather_start(part, 0, third[part], lines[part], 8)
            spread_ += gather_start(part, 1, second[part], spot[third[part]] * 8, 32)
        drain(held)
        yield
        for part in parts:
            at = [(spot[third[part]] + d) % 4 * 8 for d in range(4)]
            spread_ += gather_next(part, 0, third[part], lines[part], 8)
            spread_ += gather_start(part, 2, second[part], at[1], 32)
            spread_ += gather_start(part, 4, second[part], at[3], 32)
            spread_ += gather_next(part, 1, second[part], at[0], 32)
        yield
        for part in parts:
            at = [(spot[third[part]] + d) % 4 * 8 for d in range(4)]
            gather_end(part, 0, third[part], lines[part], 8)
            spread_ += gather_start(part, 3, second[part], at[2], 32)
            spread_ += gather_next(part, 2, second[part], at[1], 32)
            spread_ += gather_next(part, 4, second[part], at[3], 32)
        yield
        for part in parts:
            at = [(spot[third[part]] + d) % 4 * 8 for d in range(4)]
            spread_ += gather_next(part, 3, second[part], at[2], 32)
        for part in parts:
            at = [(spot[third[part]] + d) % 4 * 8 for d in range(4)]
            for d in range(4):
                gather_end(part, 1 + d, second[part], at[d], 32)
        sent = exchange_start(1, flux_slot, back, back_relay)
        yield
        sent += exchange_next(1, back, back_relay)
        drain(spread_)
        yield
        for part in parts:
            arrive(1, part, back)

        def force(group, acc):
            for one in range(4):
                r = group * 4 + one
                b = own_s[BY_SOURCE, r]
                taken = jnp.concatenate([back[part][own_s[SLOT + TABLE[part], b]] for part in parts], axis=0)
                term = jnp.dot(taken, turned[b], preferred_element_type=F32)
                term = jnp.where(lane < valid[b], term, 0.0)
                acc = acc * own_s[SAME, r].astype(F32) + term
                pre[r] = acc
            return acc

        lax.fori_loop(0, NBLK // 4, force, jnp.zeros((tall, W), F32))
        for tile in range(TILES):
            lanes = slice(tile * W, (tile + 1) * W)
            forcing = pre[own_s[END, tile]]
            change = rate[top:top + tall] * jnp.tanh(forcing)
            new = (mask[:, lanes] * (ice_t[tile].astype(F32) + change)).astype(BF16)
            ice_t[tile] = new
            if final:
                ice_out[top:top + tall, lanes] = new
        drain(sent)

    if not unrolled:
        listen()

        def whole(turn, carry):
            for half in range(count):
                for unused in run(half, True):
                    pass
            return carry

        lax.fori_loop(0, 2, whole, 0)
        conclude()
        return

    def both(half):
        yield from run(half, False)
        yield from run(half, True)

    live = [both(half) for half in range(count)]
    for at, half in enumerate(plan):
        next(live[half], None)
        if at == LISTEN:
            listen()
    for one in live:
        for unused in one:
            pass
    conclude()


def couple(cap, which, halves, unrolled, plan, src, valid, goal, source, ice, ocean, mask, rate, weights):
    cells = TILES * W
    scratch = []
    for rows in halves:
        tall = sum(rows)
        scratch += [pltpu.VMEM((TILES, tall, W), BF16), pltpu.VMEM((NBLK, tall, W), BF16), pltpu.VMEM((NBLK + 1, tall, W), F32)]
        for shape in (
            (8 * MOST,), (8 * MOST,), (2, cap), (8 * MOST,), (2, cap), (8 * MOST + 1,), (DENSE,), (DENSE,),
            (4, 2, 4), (4, 2, 8), (2, 4), (2, 8),
        ):
            scratch += [pltpu.VMEM(shape + (height, W), BF16) for height in rows]
    n = len(halves)
    scratch += [
        pltpu.VMEM((1, 1, NBLK), I32), pltpu.VMEM((3, 8, 1, NBLK), I32),
        pltpu.VMEM((OWN_ROWS, W), I32), pltpu.VMEM((GROUP_ROWS, W), I32),
        pltpu.SMEM((OWN_ROWS, W), I32), pltpu.SMEM((GROUP_ROWS, W), I32),
        pltpu.VMEM((4, 1, NBLK), I32), pltpu.VMEM((4, 1, NBLK), I32),
        pltpu.VMEM((NBLK, W, W), BF16), pltpu.VMEM((NBLK, W, W), BF16),
    ]
    scratch += [
        pltpu.SemaphoreType.DMA((n, 2, PARTS, 9)), pltpu.SemaphoreType.DMA((n, 2, PARTS, 10)),
        pltpu.SemaphoreType.DMA((n, PARTS, 5, 6)), pltpu.SemaphoreType.DMA((n, PARTS, 5, 6)),
        pltpu.SemaphoreType.DMA((n, PARTS, 5, 4)), pltpu.SemaphoreType.DMA((n, PARTS, 5, 4)),
        pltpu.SemaphoreType.DMA((5, 8)), pltpu.SemaphoreType.DMA((5, 8)), pltpu.SemaphoreType.DMA((3,)),
    ]
    vmem = pl.BlockSpec(memory_space=pltpu.VMEM)
    return pl.pallas_call(
        functools.partial(body, cap, halves, unrolled, plan),
        out_shape=(
            jax.ShapeDtypeStruct((CH, cells), BF16), jax.ShapeDtypeStruct((CH, cells), BF16), jax.ShapeDtypeStruct((1,), I32)
        ),
        in_specs=[pl.BlockSpec(memory_space=pltpu.SMEM)] * 2 + [vmem] * 6 + [pl.BlockSpec(memory_space=pl.ANY)],
        out_specs=(vmem, vmem, pl.BlockSpec(memory_space=pltpu.SMEM)),
        scratch_shapes=scratch,
        compiler_params=pltpu.CompilerParams(
            collective_id=which, has_side_effects=True, vmem_limit_bytes=66 * 1024 * 1024 - 2200000
        ),
    )(src, valid, goal, source, ice, ocean, mask, rate, weights)


def on_device(ice_state, ocean_state, ice_rate, block_weights, block_route, block_tiles, block_valid, ice_mask):
    cats, fields, cells = ice_state.shape
    chans = cats * fields
    source = block_tiles[:, 0]
    goal = (block_route[:, 0] * TILES + block_tiles[:, 1]).reshape(1, NBLK)
    ice = ice_state.reshape(chans, cells)
    ocean = ocean_state.reshape(chans, cells)
    rate = ice_rate.reshape(chans, 1)
    mask = ice_mask.astype(F32)[None, :]
    given = source, block_valid, goal, source.reshape(1, NBLK), ice, ocean, mask, rate, block_weights
    ice, flux, over = couple(FEW, 0, HALVES, True, PLAN, *given)

    def again(ice, flux, *given):
        ice, flux, unused = couple(MOST, 1, (ROWS,), False, (), *given)
        return ice, flux

    def keep(ice, flux, *given):
        return ice, flux

    ice, flux = lax.cond(over[0] > 0, again, keep, ice, flux, *given)
    return ice.reshape(cats, fields, cells), flux.reshape(cats, fields, cells)


def solution(mesh):
    placed = (
        P(None, None, ("ice", "ocn")),
        P(None, None, ("ice", "ocn")),
        P(),
        P(("ice", "ocn"), None, None),
        P(("ice", "ocn"), None),
        P(("ice", "ocn"), None),
        P(("ice", "ocn")),
        P(("ice", "ocn")),
    )
    return jax.shard_map(
        on_device,
        mesh=mesh,
        in_specs=placed,
        out_specs=(P(None, None, ("ice", "ocn")), P(None, None, ("ice", "ocn"))),
        check_vma=False,
    )
```

```python
import functools

import jax
import jax.numpy as jnp
from jax import lax
from jax.experimental import pallas as pl
from jax.experimental.pallas import tpu as pltpu
from jax.sharding import PartitionSpec as P

MESH = pl.DeviceIdType.MESH
F32 = jnp.float32
BF16 = jnp.bfloat16
I32 = jnp.int32

ROWS = (32, 32, 32, 4)
PARTS = len(ROWS)
TABLE = (0, 1, 2, 1)
HALVES = (ROWS,)
PLAN = tuple(int(one) for one in "0")
LISTEN = 0
CH = 100
NBLK = 128
TILES = 8
W = 128
MOST = 32
FEW = 20
DENSE = 128
ORDER = ((0, 1, 2), (1, 2, 0), (2, 0, 1), (1, 2, 0))


def split(owner):
    ice, ocn = owner >> 4, owner & 15
    return (ice >> 1, ocn & 3, ocn >> 2), ice & 1


def at_row(shape):
    return lax.broadcasted_iota(I32, shape, 0)


def at_lane(shape):
    return lax.broadcasted_iota(I32, shape, 1)


def down(values, keep):
    return jnp.sum(jnp.where(keep, values, 0), axis=0, keepdims=True)


def across(values, keep):
    return jnp.sum(jnp.where(keep, values, 0), axis=1, keepdims=True)


def column(row):
    n = row.shape[1]
    return across(row, at_row((n, n)) == at_lane((n, n)))


def line(col):
    n = col.shape[0]
    return down(col, at_row((n, n)) == at_lane((n, n)))


def sort_tables(key_row, key_col, count, none):
    n = key_row.shape[1]
    wide_row, wide_col = at_lane((n, n)), at_row((n, n))
    before = key_row * n + at_lane((1, n)) < key_col * n + at_row((n, 1))
    rank = across(1, before)
    hit = rank == wide_row
    perm = down(wide_col, hit)
    ordered = down(key_col, hit)
    earlier = down(key_col, rank + 1 == wide_row)
    same = jnp.where((ordered == earlier) & (at_lane((1, n)) > 0), 1, 0)
    tile = at_lane((n, W))
    upto = down(1, jnp.broadcast_to(key_col <= tile, (n, W))) - 1
    found = down(1, jnp.broadcast_to(key_col == tile, (n, W)))
    return perm, same, jnp.where(found > 0, upto, none)


def own_tables(goal, source):
    goal_col = column(goal)
    rows, most = [], jnp.zeros((1, NBLK), I32)
    earlier = at_row((NBLK, NBLK)) < at_lane((NBLK, NBLK))
    later = at_row((NBLK, NBLK)) > at_lane((NBLK, NBLK))
    blks = []
    for part in range(3):
        place, core = split(goal >> 3)
        member = place[ORDER[part][0]] * 2 + core
        place, core = split(goal_col >> 3)
        member_col = place[ORDER[part][0]] * 2 + core
        pos = down(1, (member_col == member) & earlier)
        pos_col = across(1, (member_col == member) & later)
        most = jnp.maximum(most, pos + 1)
        rows.append(member * MOST + pos)
        slot_col = member_col * MOST + pos_col
        for side in range(2):
            hit = slot_col == at_lane((NBLK, W)) + side * W
            blks.append(down(at_row((NBLK, W)), hit))
    order, same, end = sort_tables(source, column(source), TILES, NBLK)
    return rows + blks + [order, same, end], most


SLOT, BLK, BY_SOURCE, SAME, END, OWN_ROWS = 0, 3, 9, 10, 11, 16


def group_tables(part, goals, mine, my_core):
    first, second, third = ORDER[part]
    place, core = split(goals >> 3)
    picked = jnp.where((place[first] == mine[first]) & (core == my_core), 1, 0)
    dense = place[second] * 32 + place[third] * 8 + (goals & 7)
    pos = picked
    step = 1
    while step < NBLK:
        pos = pos + jnp.where(at_lane(pos.shape) >= step, pltpu.roll(pos, step, 1), 0)
        step *= 2
    pos = jnp.where(picked > 0, pos - 1, NBLK)
    k = at_row((MOST, NBLK))
    want = jnp.concatenate(
        [across(dense[m:m + 1] + 1, pos[m:m + 1] == k) for m in range(8)], axis=0) - 1
    key = jnp.where(want < 0, 1000, want)
    key_row = line(key)
    perm, keep, last = sort_tables(key_row, key, DENSE, 8 * MOST)
    want_row = jnp.where(key_row == 1000, 0, key_row)
    rows = []
    for one in (perm, keep, want_row):
        rows += [one[:, :W], one[:, W:]]
    return rows + [last]


PERM, KEEP, WANT, LAST, GROUP_ROWS = 0, 2, 4, 6, 24


def wait_in(ref, sem):
    pltpu.make_async_copy(ref, ref, sem).wait()


def body(cap, halves, unrolled, plan, src, valid, goal, source, ice_in, ocean, mask, rate, blocks, ice_out, flux_out, over, *rest):
    rest = list(rest)

    def take(count):
        out = rest[:count]
        del rest[:count]
        return out

    count = len(halves)
    a_send, a_recv, r_send, r_recv, g_send, g_recv, m_send, m_recv, t_sem = rest[-9:]
    del rest[-9:]
    said, heard, own_v, group_v, own_s, group_s, vote_y, vote_z, weights, turned, sea = rest[-11:]
    del rest[-11:]
    loading = pltpu.make_async_copy(blocks, weights, t_sem.at[2])
    loading.start()
    refs = [[take(1)[0] for unused in range(3)] + [take(PARTS) for unused in range(12)] for half in range(count)]
    my_ice, my_ocn = lax.axis_index("ice"), lax.axis_index("ocn")
    x, core = my_ice // 2, my_ice % 2
    spot = (x, my_ocn % 4, my_ocn // 4)

    def device(axis, step, which):
        place = list(spot)
        place[axis] = (place[axis] + step + 4) % 4
        return (place[0] * 2 + which, place[2] * 4 + place[1])

    def push(src, dst, send, recv, to):
        copy = pltpu.make_async_remote_copy(src, dst, send, recv, device_id=to, device_id_type=MESH)
        copy.start()
        return copy

    def drain(copies):
        for copy in copies:
            copy.wait_send()
        copies.clear()

    def loop(size, unroll, one):
        def few(k, carry):
            one(k)
            return carry

        lax.fori_loop(0, size, few, 0, unroll=unroll)

    barrier = pltpu.get_barrier_semaphore()
    peers = [(my_ice // 2 * 2 + 1 - core, my_ocn)]
    for axis in range(3):
        for step in (1, -1):
            peers += [device(axis, step, 0), device(axis, step, 1)]
        peers += [device(axis, 2, 0), device(axis, 2, 1)]
    for peer in peers:
        pl.semaphore_signal(barrier, inc=1, device_id=peer, device_id_type=MESH)
    cats, fields, unused = ice_in.shape

    def stacked(ref, lanes):
        return jnp.concatenate([ref[cat, :, lanes].astype(F32) for cat in range(cats)], axis=0)

    def unstack(ref, lanes, full):
        for cat in range(cats):
            ref[cat, :, lanes] = full[cat * fields:(cat + 1) * fields].astype(BF16)

    for tile in range(TILES):
        lanes = slice(tile * W, (tile + 1) * W)
        sea[tile] = stacked(ocean, lanes).astype(BF16)
    top = 0
    tops = []
    for half, rows in enumerate(halves):
        ice_t, prod, pre = refs[half][:3]
        tall = sum(rows)
        tops.append(top)
        for tile in range(TILES):
            lanes = slice(tile * W, (tile + 1) * W)
            ice_t[tile] = (stacked(ice_in, lanes)[top:top + tall] * mask[:, lanes]).astype(BF16)
        for part in range(PARTS):
            refs[half][8][part][8 * MOST] = jnp.zeros((rows[part], W), BF16)
        pre[NBLK] = jnp.zeros((tall, W), F32)
        top += tall
    tables, most = own_tables(goal[...], source[...])
    for row, one in enumerate(tables):
        own_v[row:row + 1] = one
    moved = pltpu.make_async_copy(own_v, own_s, t_sem.at[0])
    moved.start()
    said[0] = goal[...] + jnp.where(jnp.max(most, axis=1, keepdims=True) > cap, 1024, 0)
    for part in range(3):
        heard[part, spot[ORDER[part][0]] * 2 + core] = said[0]
    pl.semaphore_wait(barrier, len(peers))
    told = []
    for part in range(3):
        axis = ORDER[part][0]
        me = spot[axis] * 2 + core
        for turn, (step, flip) in enumerate(((0, 1), (1, 0), (1, 1), (2, 0), (2, 1), (3, 0), (3, 1))):
            other = 1 - core if flip else core
            told.append(push(
                said.at[0], heard.at[part, me], m_send.at[part, turn], m_recv.at[part, me], device(axis, step, other)))
    loading.wait()
    if not unrolled:
        moved.wait()

    def listen():
        for part in range(3):
            me = spot[ORDER[part][0]] * 2 + core
            for other in range(1, 8):
                member = (me + other) % 8
                wait_in(heard.at[part, member], m_recv.at[part, member])
            goals = jnp.concatenate([heard[part, member] for member in range(8)], axis=0)
            if part == 0:
                vote_y[spot[1]] = jnp.max(goals >> 10, axis=0, keepdims=True)
                for step in range(1, 4):
                    told.append(push(
                        vote_y.at[spot[1]], vote_y.at[spot[1]], m_send.at[3, step], m_recv.at[3, spot[1]], device(1, step, core)))
            for row, one in enumerate(group_tables(part, goals & 1023, spot, core)):
                group_v[part * 7 + row:part * 7 + row + 1] = one
        copy = pltpu.make_async_copy(group_v, group_s, t_sem.at[1])
        copy.start()
        for step in range(1, 4):
            other = (spot[1] + step) % 4
            wait_in(vote_y.at[other], m_recv.at[3, other])
        vote_z[spot[2]] = jnp.maximum(jnp.maximum(vote_y[0], vote_y[1]), jnp.maximum(vote_y[2], vote_y[3]))
        for step in range(1, 4):
            told.append(push(
                vote_z.at[spot[2]], vote_z.at[spot[2]], m_send.at[4, step], m_recv.at[4, spot[2]], device(2, step, core)))
        copy.wait()

        def turn_round(b):
            turned[b] = weights[b].T

        loop(NBLK, 4, turn_round)

    def conclude():
        for step in range(1, 4):
            other = (spot[2] + step) % 4
            wait_in(vote_z.at[other], m_recv.at[4, other])
        over[0] = jnp.max(jnp.maximum(jnp.maximum(vote_z[0], vote_z[1]), jnp.maximum(vote_z[2], vote_z[3])))
        drain(told)

    def run(half, final):
        rows, top = halves[half], tops[half]
        tall = sum(rows)
        base = [sum(rows[:part]) for part in range(PARTS)]
        ice_t, prod, pre, out_buf, in_buf, relay, back, back_relay, scan, dense, wide, rs1, rs2, rs3, rs4 = refs[half]
        lane = lax.broadcasted_iota(I32, (tall, W), 1)

        def exchange_start(way, fetch, into, hop):
            copies = []
            for part in range(PARTS):
                q = spot[ORDER[part][0]]

                members = [(q * 2 + core + other) % 8 for other in range(8)]
                lines_of = [(member // 4, member % 4 * MOST, member * MOST) for member in members]

                def fill(k, part=part, lines_of=lines_of):
                    got = [fetch(part, row, at + k) for row, at, unused in lines_of]
                    for other in range(8):
                        ref = out_buf if other else into
                        ref[part][lines_of[other][2] + k] = got[other]

                loop(cap, 2, fill)
                axis = ORDER[part][0]
                for side, step in ((0, 1), (1, -1)):
                    member = (q + 2) % 4 * 2 + side
                    copies.append(push(
                        out_buf[part].at[pl.ds(member * MOST, cap)], hop[part].at[side],
                        a_send.at[half, way, part, side], a_recv.at[half, way, part, 8 + side], device(axis, step, core)))
            for part in range(PARTS):
                axis = ORDER[part][0]
                q = spot[axis]
                me = q * 2 + core
                for turn, (step, which) in enumerate(((1, 0), (-1, 0), (1, 1), (-1, 1), (0, 1 - core))):
                    member = (q + step + 4) % 4 * 2 + which
                    copies.append(push(
                        out_buf[part].at[pl.ds(member * MOST, cap)], into[part].at[pl.ds(me * MOST, cap)],
                        a_send.at[half, way, part, 2 + turn], a_recv.at[half, way, part, me], device(axis, step, which)))
            return copies

        def exchange_next(way, into, hop):
            copies = []
            for part in range(PARTS):
                axis = ORDER[part][0]
                q = spot[axis]
                for side, step in ((0, 1), (1, -1)):
                    wait_in(hop[part].at[side], a_recv.at[half, way, part, 8 + side])
                    origin = (q - step + 4) % 4 * 2 + core
                    copies.append(push(
                        hop[part].at[side], into[part].at[pl.ds(origin * MOST, cap)],
                        a_send.at[half, way, part, 7 + side], a_recv.at[half, way, part, origin], device(axis, step, side)))
            return copies

        def arrive(way, part, into):
            q = spot[ORDER[part][0]]
            for other in range(1, 8):
                member = (q * 2 + core + other) % 8
                wait_in(into[part].at[pl.ds(member * MOST, cap)], a_recv.at[half, way, part, member])

        def scatter_far(part, key, axis, ref, at, stride, one, n):
            q, mid = spot[axis], n // 2
            far = at + (q + 2) % 4 * stride
            send, recv = r_send.at[half, part, key], r_recv.at[half, part, key]
            return [
                push(ref.at[pl.ds(far, mid)], one.at[0], send.at[0], recv.at[0], device(axis, 1, core)),
                push(ref.at[pl.ds(far + mid, mid)], one.at[1], send.at[1], recv.at[1], device(axis, -1, core)),
            ]

        def scatter_near(part, key, axis, ref, at, stride, two, n):
            q, mid = spot[axis], n // 2
            up, below = at + (q + 1) % 4 * stride, at + (q + 3) % 4 * stride
            send, recv = r_send.at[half, part, key], r_recv.at[half, part, key]
            return [
                push(ref.at[pl.ds(up + mid, mid)], two.at[0, pl.ds(mid, mid)], send.at[2], recv.at[2], device(axis, 1, core)),
                push(ref.at[pl.ds(below, mid)], two.at[1, pl.ds(0, mid)], send.at[3], recv.at[3], device(axis, -1, core)),
            ]

        def scatter_next(part, key, axis, ref, at, stride, one, two, n):
            q, mid = spot[axis], n // 2
            send, recv = r_send.at[half, part, key], r_recv.at[half, part, key]
            copies = []
            for side, step, to in ((0, 1, at + (q + 1) % 4 * stride), (1, -1, at + (q + 3) % 4 * stride + mid)):
                wait_in(one.at[side], recv.at[side])
                for k in range(mid):
                    ref[to + k] = (ref[to + k].astype(F32) + one[side, k].astype(F32)).astype(BF16)
                copies.append(push(
                    ref.at[pl.ds(to, mid)], two.at[side, pl.ds(side * mid, mid)],
                    send.at[4 + side], recv.at[4 + side], device(axis, step, core)))
            return copies

        def scatter_end(part, key, two, n):
            mid = n // 2
            recv = r_recv.at[half, part, key]
            wait_in(two.at[0, pl.ds(mid, mid)], recv.at[2])
            wait_in(two.at[1, pl.ds(0, mid)], recv.at[3])
            wait_in(two.at[0, pl.ds(0, mid)], recv.at[4])
            wait_in(two.at[1, pl.ds(mid, mid)], recv.at[5])

        def total(ref, at, two, k):
            return ref[at + k].astype(F32) + two[0, k].astype(F32) + two[1, k].astype(F32)

        def gather_start(part, key, axis, at, stride):
            q, ref = spot[axis], wide[part]
            send, recv = g_send.at[half, part, key], g_recv.at[half, part, key]
            own = ref.at[pl.ds(at + q * stride, 8)]
            return [
                push(own, own, send.at[0], recv.at[0], device(axis, 1, core)),
                push(own, own, send.at[1], recv.at[1], device(axis, -1, core)),
            ]

        def gather_next(part, key, axis, at, stride):
            q, ref = spot[axis], wide[part]
            send, recv = g_send.at[half, part, key], g_recv.at[half, part, key]
            low, high = at + (q + 3) % 4 * stride, at + (q + 1) % 4 * stride
            wait_in(ref.at[pl.ds(low, 8)], recv.at[0])
            piece = ref.at[pl.ds(low, 4)]
            first = push(piece, piece, send.at[2], recv.at[2], device(axis, 1, core))
            wait_in(ref.at[pl.ds(high, 8)], recv.at[1])
            piece = ref.at[pl.ds(high + 4, 4)]
            return [first, push(piece, piece, send.at[3], recv.at[3], device(axis, -1, core))]

        def gather_end(part, key, axis, at, stride):
            q, ref = spot[axis], wide[part]
            recv = g_recv.at[half, part, key]
            far = at + (q + 2) % 4 * stride
            wait_in(ref.at[pl.ds(far, 4)], recv.at[2])
            wait_in(ref.at[pl.ds(far + 4, 4)], recv.at[3])

        def product(b):
            tile = ice_t[src[b]]
            tile = jnp.where(lane < valid[b], tile, jnp.zeros((), BF16))
            prod[b] = jnp.dot(tile, weights[b], preferred_element_type=F32).astype(BF16)

        def product_slot(part, row, at):
            return prod[own_s[BLK + 2 * TABLE[part] + row, at], pl.ds(base[part], rows[part])]

        def flux_slot(part, row, at):
            return wide[part][group_s[7 * TABLE[part] + WANT + row, at]]

        parts = range(PARTS)
        second, third = [ORDER[part][1] for part in parts], [ORDER[part][2] for part in parts]
        lines = [spot[second[part]] * 32 for part in parts]
        loop(NBLK, 8, product)
        if unrolled and not final and half == 0:
            moved.wait()
        sent = exchange_start(0, product_slot, in_buf, relay)
        yield
        sent += exchange_next(0, in_buf, relay)
        yield
        held = []
        for part in parts:
            arrive(0, part, in_buf)
            acc = jnp.zeros((rows[part], W), F32)
            for line_, steps in ((0, min(W, 8 * cap)), (1, 8 * cap - W)):
                def add(group, acc, part=part, line_=line_):
                    for one in range(8):
                        r = group * 8 + one
                        piece = in_buf[part][group_s[7 * TABLE[part] + PERM + line_, r]].astype(F32)
                        acc = acc * group_s[7 * TABLE[part] + KEEP + line_, r].astype(F32) + piece
                        scan[part][line_ * W + r] = acc.astype(BF16)
                    return acc

                acc = lax.fori_loop(0, steps // 8, add, acc)
            for d in (2, 1, 3, 0):
                at = (spot[third[part]] + d) % 4 * 8

                def settle(k, part=part, at=at):
                    got = [scan[part][group_s[7 * TABLE[part] + LAST, k * 32 + at + tile]] for tile in range(8)]
                    for tile in range(8):
                        dense[part][k * 32 + at + tile] = got[tile]

                loop(4, 1, settle)
                held += scatter_far(part, 1 + d, second[part], dense[part], at, 32, rs1[part].at[d], 8)
                held += scatter_near(part, 1 + d, second[part], dense[part], at, 32, rs2[part].at[d], 8)
        yield
        for d in (2, 1, 3, 0):
            for part in parts:
                at = (spot[third[part]] + d) % 4 * 8
                held += scatter_next(part, 1 + d, second[part], dense[part], at, 32, rs1[part].at[d], rs2[part].at[d], 8)
        yield

        def collect(part, d):
            scatter_end(part, 1 + d, rs2[part].at[d], 8)
            at = lines[part] + (spot[third[part]] + d) % 4 * 8
            for k in range(8):
                dense[part][at + k] = total(dense[part], at, rs2[part].at[d], k).astype(BF16)

        for part in parts:
            collect(part, 2)
            held += scatter_far(part, 0, third[part], dense[part], lines[part], 8, rs3[part], 8)
        for part in parts:
            collect(part, 1)
            collect(part, 3)
            held += scatter_near(part, 0, third[part], dense[part], lines[part], 8, rs4[part], 8)
        yield
        for part in parts:
            held += scatter_next(part, 0, third[part], dense[part], lines[part], 8, rs3[part], rs4[part], 8)
        for part in parts:
            collect(part, 0)
        drain(sent)
        yield
        spread_ = []
        for part in parts:
            scatter_end(part, 0, rs4[part], 8)
            at = lines[part] + spot[third[part]] * 8
            here = slice(top + base[part], top + base[part] + rows[part])
            for tile in range(TILES):
                come = total(dense[part], at, rs4[part], tile)
                wide[part][at + tile] = jnp.tanh(come + sea[tile, here].astype(F32)).astype(BF16)
            spread_ += gather_start(part, 0, third[part], lines[part], 8)
            spread_ += gather_start(part, 1, second[part], spot[third[part]] * 8, 32)
        drain(held)
        yield
        for part in parts:
            at = [(spot[third[part]] + d) % 4 * 8 for d in range(4)]
            spread_ += gather_next(part, 0, third[part], lines[part], 8)
            spread_ += gather_start(part, 2, second[part], at[1], 32)
            spread_ += gather_start(part, 4, second[part], at[3], 32)
            spread_ += gather_next(part, 1, second[part], at[0], 32)
        yield
        for part in parts:
            at = [(spot[third[part]] + d) % 4 * 8 for d in range(4)]
            gather_end(part, 0, third[part], lines[part], 8)
            spread_ += gather_start(part, 3, second[part], at[2], 32)
            spread_ += gather_next(part, 2, second[part], at[1], 32)
            spread_ += gather_next(part, 4, second[part], at[3], 32)
        yield
        for part in parts:
            at = [(spot[third[part]] + d) % 4 * 8 for d in range(4)]
            spread_ += gather_next(part, 3, second[part], at[2], 32)
        for part in parts:
            at = [(spot[third[part]] + d) % 4 * 8 for d in range(4)]
            for d in range(4):
                gather_end(part, 1 + d, second[part], at[d], 32)
        sent = exchange_start(1, flux_slot, back, back_relay)
        yield
        sent += exchange_next(1, back, back_relay)
        drain(spread_)
        yield
        for part in parts:
            arrive(1, part, back)

        def force(group, acc):
            for one in range(4):
                r = group * 4 + one
                b = own_s[BY_SOURCE, r]
                taken = jnp.concatenate([back[part][own_s[SLOT + TABLE[part], b]] for part in parts], axis=0)
                term = jnp.dot(taken, turned[b], preferred_element_type=F32)
                term = jnp.where(lane < valid[b], term, 0.0)
                acc = acc * own_s[SAME, r].astype(F32) + term
                pre[r] = acc
            return acc

        lax.fori_loop(0, NBLK // 4, force, jnp.zeros((tall, W), F32))
        for tile in range(TILES):
            lanes = slice(tile * W, (tile + 1) * W)
            forcing = pre[own_s[END, tile]]
            change = rate[top:top + tall] * jnp.tanh(forcing)
            new = (mask[:, lanes] * (ice_t[tile].astype(F32) + change)).astype(BF16)
            ice_t[tile] = new
            if final:
                unstack(ice_out, lanes, new.astype(F32))
                full = [wide[part][lines[part] + spot[third[part]] * 8 + tile].astype(F32) for part in parts]
                unstack(flux_out, lanes, jnp.concatenate(full, axis=0))
        drain(sent)

    if not unrolled:
        listen()

        def whole(turn, carry):
            for half in range(count):
                for unused in run(half, True):
                    pass
            return carry

        lax.fori_loop(0, 2, whole, 0)
        conclude()
        return

    def both(half):
        yield from run(half, False)
        yield from run(half, True)

    live = [both(half) for half in range(count)]
    for at, half in enumerate(plan):
        next(live[half], None)
        if at == LISTEN:
            listen()
    for one in live:
        for unused in one:
            pass
    conclude()


def couple(cap, which, halves, unrolled, plan, src, valid, goal, source, ice, ocean, mask, rate, weights):
    result = jax.ShapeDtypeStruct(ice.shape, BF16)
    scratch = []
    for rows in halves:
        tall = sum(rows)
        scratch += [pltpu.VMEM((TILES, tall, W), BF16), pltpu.VMEM((NBLK, tall, W), BF16), pltpu.VMEM((NBLK + 1, tall, W), F32)]
        for shape in (
            (8 * MOST,), (8 * MOST,), (2, cap), (8 * MOST,), (2, cap), (8 * MOST + 1,), (DENSE,), (DENSE,),
            (4, 2, 4), (4, 2, 8), (2, 4), (2, 8),
        ):
            scratch += [pltpu.VMEM(shape + (height, W), BF16) for height in rows]
    n = len(halves)
    scratch += [
        pltpu.VMEM((1, 1, NBLK), I32), pltpu.VMEM((3, 8, 1, NBLK), I32),
        pltpu.VMEM((OWN_ROWS, W), I32), pltpu.VMEM((GROUP_ROWS, W), I32),
        pltpu.SMEM((OWN_ROWS, W), I32), pltpu.SMEM((GROUP_ROWS, W), I32),
        pltpu.VMEM((4, 1, NBLK), I32), pltpu.VMEM((4, 1, NBLK), I32),
        pltpu.VMEM((NBLK, W, W), BF16), pltpu.VMEM((NBLK, W, W), BF16), pltpu.VMEM((TILES, CH, W), BF16),
    ]
    scratch += [
        pltpu.SemaphoreType.DMA((n, 2, PARTS, 9)), pltpu.SemaphoreType.DMA((n, 2, PARTS, 10)),
        pltpu.SemaphoreType.DMA((n, PARTS, 5, 6)), pltpu.SemaphoreType.DMA((n, PARTS, 5, 6)),
        pltpu.SemaphoreType.DMA((n, PARTS, 5, 4)), pltpu.SemaphoreType.DMA((n, PARTS, 5, 4)),
        pltpu.SemaphoreType.DMA((5, 8)), pltpu.SemaphoreType.DMA((5, 8)), pltpu.SemaphoreType.DMA((3,)),
    ]
    vmem = pl.BlockSpec(memory_space=pltpu.VMEM)
    return pl.pallas_call(
        functools.partial(body, cap, halves, unrolled, plan),
        out_shape=(
            result, result, jax.ShapeDtypeStruct((1,), I32)
        ),
        in_specs=[pl.BlockSpec(memory_space=pltpu.SMEM)] * 2 + [vmem] * 6 + [pl.BlockSpec(memory_space=pl.ANY)],
        out_specs=(vmem, vmem, pl.BlockSpec(memory_space=pltpu.SMEM)),
        scratch_shapes=scratch,
        compiler_params=pltpu.CompilerParams(
            collective_id=which, has_side_effects=True, vmem_limit_bytes=66 * 1024 * 1024 - 2200000
        ),
    )(src, valid, goal, source, ice, ocean, mask, rate, weights)


def on_device(ice_state, ocean_state, ice_rate, block_weights, block_route, block_tiles, block_valid, ice_mask):
    cats, fields, cells = ice_state.shape
    chans = cats * fields
    source = block_tiles[:, 0]
    goal = (block_route[:, 0] * TILES + block_tiles[:, 1]).reshape(1, NBLK)
    rate = ice_rate.reshape(chans, 1)
    mask = ice_mask.astype(F32)[None, :]
    given = source, block_valid, goal, source.reshape(1, NBLK), ice_state, ocean_state, mask, rate, block_weights
    ice, flux, over = couple(FEW, 0, HALVES, True, PLAN, *given)

    def again(ice, flux, *given):
        ice, flux, unused = couple(MOST, 1, (ROWS,), False, (), *given)
        return ice, flux

    def keep(ice, flux, *given):
        return ice, flux

    ice, flux = lax.cond(over[0] > 0, again, keep, ice, flux, *given)
    return ice, flux


def solution(mesh):
    placed = (
        P(None, None, ("ice", "ocn")),
        P(None, None, ("ice", "ocn")),
        P(),
        P(("ice", "ocn"), None, None),
        P(("ice", "ocn"), None),
        P(("ice", "ocn"), None),
        P(("ice", "ocn")),
        P(("ice", "ocn")),
    )
    return jax.shard_map(
        on_device,
        mesh=mesh,
        in_specs=placed,
        out_specs=(P(None, None, ("ice", "ocn")), P(None, None, ("ice", "ocn"))),
        check_vma=False,
    )
```

```python
import functools

import jax
import jax.numpy as jnp
from jax import lax
from jax.experimental import pallas as pl
from jax.experimental.pallas import tpu as pltpu
from jax.sharding import PartitionSpec as P

MESH = pl.DeviceIdType.MESH
F32 = jnp.float32
BF16 = jnp.bfloat16
I32 = jnp.int32

ROWS = (32, 32, 32, 4)
PARTS = len(ROWS)
TABLE = (0, 1, 2, 1)
HALVES = (ROWS,)
PLAN = tuple(int(one) for one in "0")
LISTEN = 0
CH = 100
NBLK = 128
TILES = 8
W = 128
MOST = 32
FEW = 20
DENSE = 128
ORDER = ((0, 1, 2), (1, 2, 0), (2, 0, 1), (1, 2, 0))


def split(owner):
    ice, ocn = owner >> 4, owner & 15
    return (ice >> 1, ocn & 3, ocn >> 2), ice & 1


def at_row(shape):
    return lax.broadcasted_iota(I32, shape, 0)


def at_lane(shape):
    return lax.broadcasted_iota(I32, shape, 1)


def down(values, keep):
    return jnp.sum(jnp.where(keep, values, 0), axis=0, keepdims=True)


def across(values, keep):
    return jnp.sum(jnp.where(keep, values, 0), axis=1, keepdims=True)


def column(row):
    n = row.shape[1]
    return across(row, at_row((n, n)) == at_lane((n, n)))


def line(col):
    n = col.shape[0]
    return down(col, at_row((n, n)) == at_lane((n, n)))


def sort_tables(key_row, key_col, count, none):
    n = key_row.shape[1]
    wide_row, wide_col = at_lane((n, n)), at_row((n, n))
    before = key_row * n + at_lane((1, n)) < key_col * n + at_row((n, 1))
    rank = across(1, before)
    hit = rank == wide_row
    perm = down(wide_col, hit)
    ordered = down(key_col, hit)
    earlier = down(key_col, rank + 1 == wide_row)
    same = jnp.where((ordered == earlier) & (at_lane((1, n)) > 0), 1, 0)
    tile = at_lane((n, W))
    upto = down(1, jnp.broadcast_to(key_col <= tile, (n, W))) - 1
    found = down(1, jnp.broadcast_to(key_col == tile, (n, W)))
    return perm, same, jnp.where(found > 0, upto, none)


def own_tables(goal, source):
    goal_col = column(goal)
    rows, most = [], jnp.zeros((1, NBLK), I32)
    earlier = at_row((NBLK, NBLK)) < at_lane((NBLK, NBLK))
    later = at_row((NBLK, NBLK)) > at_lane((NBLK, NBLK))
    blks = []
    for part in range(3):
        place, core = split(goal >> 3)
        member = place[ORDER[part][0]] * 2 + core
        place, core = split(goal_col >> 3)
        member_col = place[ORDER[part][0]] * 2 + core
        pos = down(1, (member_col == member) & earlier)
        pos_col = across(1, (member_col == member) & later)
        most = jnp.maximum(most, pos + 1)
        rows.append(member * MOST + pos)
        slot_col = member_col * MOST + pos_col
        for side in range(2):
            hit = slot_col == at_lane((NBLK, W)) + side * W
            blks.append(down(at_row((NBLK, W)), hit))
    order, same, end = sort_tables(source, column(source), TILES, NBLK)
    return rows + blks + [order, same, end], most


SLOT, BLK, BY_SOURCE, SAME, END, OWN_ROWS = 0, 3, 9, 10, 11, 16


def group_tables(part, goals, mine, my_core):
    first, second, third = ORDER[part]
    place, core = split(goals >> 3)
    picked = jnp.where((place[first] == mine[first]) & (core == my_core), 1, 0)
    dense = place[second] * 32 + place[third] * 8 + (goals & 7)
    pos = picked
    step = 1
    while step < NBLK:
        pos = pos + jnp.where(at_lane(pos.shape) >= step, pltpu.roll(pos, step, 1), 0)
        step *= 2
    pos = jnp.where(picked > 0, pos - 1, NBLK)
    k = at_row((MOST, NBLK))
    want = jnp.concatenate(
        [across(dense[m:m + 1] + 1, pos[m:m + 1] == k) for m in range(8)], axis=0) - 1
    key = jnp.where(want < 0, 1000, want)
    key_row = line(key)
    perm, keep, last = sort_tables(key_row, key, DENSE, 8 * MOST)
    want_row = jnp.where(key_row == 1000, 0, key_row)
    rows = []
    for one in (perm, keep, want_row):
        rows += [one[:, :W], one[:, W:]]
    return rows + [last]


PERM, KEEP, WANT, LAST, GROUP_ROWS = 0, 2, 4, 6, 24


def wait_in(ref, sem):
    pltpu.make_async_copy(ref, ref, sem).wait()


def body(cap, halves, unrolled, plan, src, valid, goal, source, ice_in, ocean, mask, rate, blocks, ice_out, flux_out, over, *rest):
    rest = list(rest)

    def take(count):
        out = rest[:count]
        del rest[:count]
        return out

    count = len(halves)
    a_send, a_recv, r_send, r_recv, g_send, g_recv, m_send, m_recv, t_sem = rest[-9:]
    del rest[-9:]
    said, heard, own_v, group_v, own_s, group_s, vote_y, vote_z, weights, turned, sea = rest[-11:]
    del rest[-11:]
    loading = pltpu.make_async_copy(blocks, weights, t_sem.at[2])
    loading.start()
    refs = [[take(1)[0] for unused in range(3)] + [take(PARTS) for unused in range(12)] for half in range(count)]
    my_ice, my_ocn = lax.axis_index("ice"), lax.axis_index("ocn")
    x, core = my_ice // 2, my_ice % 2
    spot = (x, my_ocn % 4, my_ocn // 4)

    def device(axis, step, which):
        place = list(spot)
        place[axis] = (place[axis] + step + 4) % 4
        return (place[0] * 2 + which, place[2] * 4 + place[1])

    def push(src, dst, send, recv, to):
        copy = pltpu.make_async_remote_copy(src, dst, send, recv, device_id=to, device_id_type=MESH)
        copy.start()
        return copy

    def drain(copies):
        for copy in copies:
            copy.wait_send()
        copies.clear()

    def loop(size, unroll, one):
        def few(k, carry):
            one(k)
            return carry

        lax.fori_loop(0, size, few, 0, unroll=unroll)

    barrier = pltpu.get_barrier_semaphore()
    peers = [(my_ice // 2 * 2 + 1 - core, my_ocn)]
    for axis in range(3):
        for step in (1, -1):
            peers += [device(axis, step, 0), device(axis, step, 1)]
        peers += [device(axis, 2, 0), device(axis, 2, 1)]
    for peer in peers:
        pl.semaphore_signal(barrier, inc=1, device_id=peer, device_id_type=MESH)
    cats, fields, unused = ice_in.shape

    def stacked(ref, lanes):
        return jnp.concatenate([ref[cat, :, lanes].astype(F32) for cat in range(cats)], axis=0)

    def unstack(ref, lanes, full):
        for cat in range(cats):
            ref[cat, :, lanes] = full[cat * fields:(cat + 1) * fields].astype(BF16)

    for tile in range(TILES):
        lanes = slice(tile * W, (tile + 1) * W)
        sea[tile] = stacked(ocean, lanes).astype(BF16)
    top = 0
    tops = []
    for half, rows in enumerate(halves):
        ice_t, prod, pre = refs[half][:3]
        tall = sum(rows)
        tops.append(top)
        for tile in range(TILES):
            lanes = slice(tile * W, (tile + 1) * W)
            ice_t[tile] = (stacked(ice_in, lanes)[top:top + tall] * mask[:, lanes]).astype(BF16)
        for part in range(PARTS):
            refs[half][8][part][8 * MOST] = jnp.zeros((rows[part], W), BF16)
        pre[NBLK] = jnp.zeros((tall, W), F32)
        top += tall
    tables, most = own_tables(goal[...], source[...])
    for row, one in enumerate(tables):
        own_v[row:row + 1] = one
    moved = pltpu.make_async_copy(own_v, own_s, t_sem.at[0])
    moved.start()
    said[0] = goal[...] + jnp.where(jnp.max(most, axis=1, keepdims=True) > cap, 1024, 0)
    for part in range(3):
        heard[part, spot[ORDER[part][0]] * 2 + core] = said[0]
    pl.semaphore_wait(barrier, len(peers))
    told = []
    for part in range(3):
        axis = ORDER[part][0]
        me = spot[axis] * 2 + core
        for turn, (step, flip) in enumerate(((0, 1), (1, 0), (1, 1), (2, 0), (2, 1), (3, 0), (3, 1))):
            other = 1 - core if flip else core
            told.append(push(
                said.at[0], heard.at[part, me], m_send.at[part, turn], m_recv.at[part, me], device(axis, step, other)))
    loading.wait()
    if not unrolled:
        moved.wait()

    def listen():
        for part in range(3):
            me = spot[ORDER[part][0]] * 2 + core
            for other in range(1, 8):
                member = (me + other) % 8
                wait_in(heard.at[part, member], m_recv.at[part, member])
            goals = jnp.concatenate([heard[part, member] for member in range(8)], axis=0)
            if part == 0:
                vote_y[spot[1]] = jnp.max(goals >> 10, axis=0, keepdims=True)
                for step in range(1, 4):
                    told.append(push(
                        vote_y.at[spot[1]], vote_y.at[spot[1]], m_send.at[3, step], m_recv.at[3, spot[1]], device(1, step, core)))
            for row, one in enumerate(group_tables(part, goals & 1023, spot, core)):
                group_v[part * 7 + row:part * 7 + row + 1] = one
        copy = pltpu.make_async_copy(group_v, group_s, t_sem.at[1])
        copy.start()
        for step in range(1, 4):
            other = (spot[1] + step) % 4
            wait_in(vote_y.at[other], m_recv.at[3, other])
        vote_z[spot[2]] = jnp.maximum(jnp.maximum(vote_y[0], vote_y[1]), jnp.maximum(vote_y[2], vote_y[3]))
        for step in range(1, 4):
            told.append(push(
                vote_z.at[spot[2]], vote_z.at[spot[2]], m_send.at[4, step], m_recv.at[4, spot[2]], device(2, step, core)))
        copy.wait()

        def turn_round(b):
            turned[b] = weights[b].T

        loop(NBLK, 4, turn_round)

    def conclude():
        for step in range(1, 4):
            other = (spot[2] + step) % 4
            wait_in(vote_z.at[other], m_recv.at[4, other])
        over[0] = jnp.max(jnp.maximum(jnp.maximum(vote_z[0], vote_z[1]), jnp.maximum(vote_z[2], vote_z[3])))
        drain(told)

    def run(half, final):
        rows, top = halves[half], tops[half]
        tall = sum(rows)
        base = [sum(rows[:part]) for part in range(PARTS)]
        ice_t, prod, pre, out_buf, in_buf, relay, back, back_relay, scan, dense, wide, rs1, rs2, rs3, rs4 = refs[half]
        lane = lax.broadcasted_iota(I32, (tall, W), 1)

        def exchange_start(way, fetch, into, hop, ready=None):
            copies = []
            for part in range(PARTS):
                q = spot[ORDER[part][0]]
                if ready:
                    ready(part)
                members = [(q * 2 + core + other) % 8 for other in range(8)]
                lines_of = [(member // 4, member % 4 * MOST, member * MOST) for member in members]

                def fill(k, part=part, lines_of=lines_of):
                    got = [fetch(part, row, at + k) for row, at, unused in lines_of]
                    for other in range(8):
                        ref = out_buf if other else into
                        ref[part][lines_of[other][2] + k] = got[other]

                loop(cap, 2, fill)
                axis = ORDER[part][0]
                for side, step in ((0, 1), (1, -1)):
                    member = (q + 2) % 4 * 2 + side
                    copies.append(push(
                        out_buf[part].at[pl.ds(member * MOST, cap)], hop[part].at[side],
                        a_send.at[half, way, part, side], a_recv.at[half, way, part, 8 + side], device(axis, step, core)))
            for part in range(PARTS):
                axis = ORDER[part][0]
                q = spot[axis]
                me = q * 2 + core
                for turn, (step, which) in enumerate(((1, 0), (-1, 0), (1, 1), (-1, 1), (0, 1 - core))):
                    member = (q + step + 4) % 4 * 2 + which
                    copies.append(push(
                        out_buf[part].at[pl.ds(member * MOST, cap)], into[part].at[pl.ds(me * MOST, cap)],
                        a_send.at[half, way, part, 2 + turn], a_recv.at[half, way, part, me], device(axis, step, which)))
            return copies

        def exchange_next(way, into, hop):
            copies = []
            for part in range(PARTS):
                axis = ORDER[part][0]
                q = spot[axis]
                for side, step in ((0, 1), (1, -1)):
                    wait_in(hop[part].at[side], a_recv.at[half, way, part, 8 + side])
                    origin = (q - step + 4) % 4 * 2 + core
                    copies.append(push(
                        hop[part].at[side], into[part].at[pl.ds(origin * MOST, cap)],
                        a_send.at[half, way, part, 7 + side], a_recv.at[half, way, part, origin], device(axis, step, side)))
            return copies

        def arrive(way, part, into):
            q = spot[ORDER[part][0]]
            for other in range(1, 8):
                member = (q * 2 + core + other) % 8
                wait_in(into[part].at[pl.ds(member * MOST, cap)], a_recv.at[half, way, part, member])

        def scatter_far(part, key, axis, ref, at, stride, one, n):
            q, mid = spot[axis], n // 2
            far = at + (q + 2) % 4 * stride
            send, recv = r_send.at[half, part, key], r_recv.at[half, part, key]
            return [
                push(ref.at[pl.ds(far, mid)], one.at[0], send.at[0], recv.at[0], device(axis, 1, core)),
                push(ref.at[pl.ds(far + mid, mid)], one.at[1], send.at[1], recv.at[1], device(axis, -1, core)),
            ]

        def scatter_near(part, key, axis, ref, at, stride, two, n):
            q, mid = spot[axis], n // 2
            up, below = at + (q + 1) % 4 * stride, at + (q + 3) % 4 * stride
            send, recv = r_send.at[half, part, key], r_recv.at[half, part, key]
            return [
                push(ref.at[pl.ds(up + mid, mid)], two.at[0, pl.ds(mid, mid)], send.at[2], recv.at[2], device(axis, 1, core)),
                push(ref.at[pl.ds(below, mid)], two.at[1, pl.ds(0, mid)], send.at[3], recv.at[3], device(axis, -1, core)),
            ]

        def scatter_next(part, key, axis, ref, at, stride, one, two, n):
            q, mid = spot[axis], n // 2
            send, recv = r_send.at[half, part, key], r_recv.at[half, part, key]
            copies = []
            for side, step, to in ((0, 1, at + (q + 1) % 4 * stride), (1, -1, at + (q + 3) % 4 * stride + mid)):
                wait_in(one.at[side], recv.at[side])
                for k in range(mid):
                    ref[to + k] = (ref[to + k].astype(F32) + one[side, k].astype(F32)).astype(BF16)
                copies.append(push(
                    ref.at[pl.ds(to, mid)], two.at[side, pl.ds(side * mid, mid)],
                    send.at[4 + side], recv.at[4 + side], device(axis, step, core)))
            return copies

        def scatter_end(part, key, two, n):
            mid = n // 2
            recv = r_recv.at[half, part, key]
            wait_in(two.at[0, pl.ds(mid, mid)], recv.at[2])
            wait_in(two.at[1, pl.ds(0, mid)], recv.at[3])
            wait_in(two.at[0, pl.ds(0, mid)], recv.at[4])
            wait_in(two.at[1, pl.ds(mid, mid)], recv.at[5])

        def total(ref, at, two, k):
            return ref[at + k].astype(F32) + two[0, k].astype(F32) + two[1, k].astype(F32)

        def gather_start(part, key, axis, at, stride):
            q, ref = spot[axis], wide[part]
            send, recv = g_send.at[half, part, key], g_recv.at[half, part, key]
            own = ref.at[pl.ds(at + q * stride, 8)]
            return [
                push(own, own, send.at[0], recv.at[0], device(axis, 1, core)),
                push(own, own, send.at[1], recv.at[1], device(axis, -1, core)),
            ]

        def gather_next(part, key, axis, at, stride):
            q, ref = spot[axis], wide[part]
            send, recv = g_send.at[half, part, key], g_recv.at[half, part, key]
            low, high = at + (q + 3) % 4 * stride, at + (q + 1) % 4 * stride
            wait_in(ref.at[pl.ds(low, 8)], recv.at[0])
            piece = ref.at[pl.ds(low, 4)]
            first = push(piece, piece, send.at[2], recv.at[2], device(axis, 1, core))
            wait_in(ref.at[pl.ds(high, 8)], recv.at[1])
            piece = ref.at[pl.ds(high + 4, 4)]
            return [first, push(piece, piece, send.at[3], recv.at[3], device(axis, -1, core))]

        def gather_end(part, key, axis, at, stride):
            q, ref = spot[axis], wide[part]
            recv = g_recv.at[half, part, key]
            far = at + (q + 2) % 4 * stride
            wait_in(ref.at[pl.ds(far, 4)], recv.at[2])
            wait_in(ref.at[pl.ds(far + 4, 4)], recv.at[3])

        def product(b):
            tile = ice_t[src[b]]
            tile = jnp.where(lane < valid[b], tile, jnp.zeros((), BF16))
            prod[b] = jnp.dot(tile, weights[b], preferred_element_type=F32).astype(BF16)

        def product_slot(part, row, at):
            return prod[own_s[BLK + 2 * TABLE[part] + row, at], pl.ds(base[part], rows[part])]

        def flux_slot(part, row, at):
            return wide[part][group_s[7 * TABLE[part] + WANT + row, at]]

        parts = range(PARTS)
        second, third = [ORDER[part][1] for part in parts], [ORDER[part][2] for part in parts]
        lines = [spot[second[part]] * 32 for part in parts]
        loop(NBLK, 8, product)
        if unrolled and not final and half == 0:
            moved.wait()
        sent = exchange_start(0, product_slot, in_buf, relay)
        yield
        sent += exchange_next(0, in_buf, relay)
        yield
        held = []
        for part in parts:
            arrive(0, part, in_buf)
            acc = jnp.zeros((rows[part], W), F32)
            for line_, steps in ((0, min(W, 8 * cap)), (1, 8 * cap - W)):
                def add(group, acc, part=part, line_=line_):
                    for one in range(8):
                        r = group * 8 + one
                        piece = in_buf[part][group_s[7 * TABLE[part] + PERM + line_, r]].astype(F32)
                        acc = acc * group_s[7 * TABLE[part] + KEEP + line_, r].astype(F32) + piece
                        scan[part][line_ * W + r] = acc.astype(BF16)
                    return acc

                acc = lax.fori_loop(0, steps // 8, add, acc)
            for d in (2, 1, 3, 0):
                at = (spot[third[part]] + d) % 4 * 8

                def settle(k, part=part, at=at):
                    got = [scan[part][group_s[7 * TABLE[part] + LAST, k * 32 + at + tile]] for tile in range(8)]
                    for tile in range(8):
                        dense[part][k * 32 + at + tile] = got[tile]

                loop(4, 1, settle)
                held += scatter_far(part, 1 + d, second[part], dense[part], at, 32, rs1[part].at[d], 8)
                held += scatter_near(part, 1 + d, second[part], dense[part], at, 32, rs2[part].at[d], 8)
        yield
        for d in (2, 1, 3, 0):
            for part in parts:
                at = (spot[third[part]] + d) % 4 * 8
                held += scatter_next(part, 1 + d, second[part], dense[part], at, 32, rs1[part].at[d], rs2[part].at[d], 8)
        yield

        def collect(part, d):
            scatter_end(part, 1 + d, rs2[part].at[d], 8)
            at = lines[part] + (spot[third[part]] + d) % 4 * 8
            for k in range(8):
                dense[part][at + k] = total(dense[part], at, rs2[part].at[d], k).astype(BF16)

        for part in parts:
            collect(part, 2)
            held += scatter_far(part, 0, third[part], dense[part], lines[part], 8, rs3[part], 8)
        for part in parts:
            collect(part, 1)
            collect(part, 3)
            held += scatter_near(part, 0, third[part], dense[part], lines[part], 8, rs4[part], 8)
        yield
        for part in parts:
            held += scatter_next(part, 0, third[part], dense[part], lines[part], 8, rs3[part], rs4[part], 8)
        for part in parts:
            collect(part, 0)
        drain(sent)
        yield
        spread_ = []
        for part in parts:
            scatter_end(part, 0, rs4[part], 8)
            at = lines[part] + spot[third[part]] * 8
            here = slice(top + base[part], top + base[part] + rows[part])
            for tile in range(TILES):
                come = total(dense[part], at, rs4[part], tile)
                wide[part][at + tile] = jnp.tanh(come + sea[tile, here].astype(F32)).astype(BF16)
            spread_ += gather_start(part, 0, third[part], lines[part], 8)
            spread_ += gather_start(part, 1, second[part], spot[third[part]] * 8, 32)
        drain(held)
        yield
        for part in parts:
            at = [(spot[third[part]] + d) % 4 * 8 for d in range(4)]
            spread_ += gather_next(part, 0, third[part], lines[part], 8)
            spread_ += gather_start(part, 2, second[part], at[1], 32)
            spread_ += gather_start(part, 4, second[part], at[3], 32)
            spread_ += gather_next(part, 1, second[part], at[0], 32)
        yield
        for part in parts:
            at = [(spot[third[part]] + d) % 4 * 8 for d in range(4)]
            gather_end(part, 0, third[part], lines[part], 8)
            spread_ += gather_start(part, 3, second[part], at[2], 32)
            spread_ += gather_next(part, 2, second[part], at[1], 32)
            spread_ += gather_next(part, 4, second[part], at[3], 32)
        yield
        for part in parts:
            at = [(spot[third[part]] + d) % 4 * 8 for d in range(4)]
            spread_ += gather_next(part, 3, second[part], at[2], 32)

        def gathered(part):
            for d in range(4):
                gather_end(part, 1 + d, second[part], (spot[third[part]] + d) % 4 * 8, 32)

        sent = exchange_start(1, flux_slot, back, back_relay, gathered)
        yield
        sent += exchange_next(1, back, back_relay)
        drain(spread_)
        yield
        for part in parts:
            arrive(1, part, back)

        def force(group, acc):
            for one in range(4):
                r = group * 4 + one
                b = own_s[BY_SOURCE, r]
                taken = jnp.concatenate([back[part][own_s[SLOT + TABLE[part], b]] for part in parts], axis=0)
                term = jnp.dot(taken, turned[b], preferred_element_type=F32)
                term = jnp.where(lane < valid[b], term, 0.0)
                acc = acc * own_s[SAME, r].astype(F32) + term
                pre[r] = acc
            return acc

        lax.fori_loop(0, NBLK // 4, force, jnp.zeros((tall, W), F32))
        for tile in range(TILES):
            lanes = slice(tile * W, (tile + 1) * W)
            forcing = pre[own_s[END, tile]]
            change = rate[top:top + tall] * jnp.tanh(forcing)
            new = (mask[:, lanes] * (ice_t[tile].astype(F32) + change)).astype(BF16)
            ice_t[tile] = new
            if final:
                unstack(ice_out, lanes, new.astype(F32))
                full = [wide[part][lines[part] + spot[third[part]] * 8 + tile].astype(F32) for part in parts]
                unstack(flux_out, lanes, jnp.concatenate(full, axis=0))
        drain(sent)

    if not unrolled:
        listen()

        def whole(turn, carry):
            for half in range(count):
                for unused in run(half, True):
                    pass
            return carry

        lax.fori_loop(0, 2, whole, 0)
        conclude()
        return

    def both(half):
        yield from run(half, False)
        yield from run(half, True)

    live = [both(half) for half in range(count)]
    for at, half in enumerate(plan):
        next(live[half], None)
        if at == LISTEN:
            listen()
    for one in live:
        for unused in one:
            pass
    conclude()


def couple(cap, which, halves, unrolled, plan, src, valid, goal, source, ice, ocean, mask, rate, weights):
    result = jax.ShapeDtypeStruct(ice.shape, BF16)
    scratch = []
    for rows in halves:
        tall = sum(rows)
        scratch += [pltpu.VMEM((TILES, tall, W), BF16), pltpu.VMEM((NBLK, tall, W), BF16), pltpu.VMEM((NBLK + 1, tall, W), F32)]
        for shape in (
            (8 * MOST,), (8 * MOST,), (2, cap), (8 * MOST,), (2, cap), (8 * MOST + 1,), (DENSE,), (DENSE,),
            (4, 2, 4), (4, 2, 8), (2, 4), (2, 8),
        ):
            scratch += [pltpu.VMEM(shape + (height, W), BF16) for height in rows]
    n = len(halves)
    scratch += [
        pltpu.VMEM((1, 1, NBLK), I32), pltpu.VMEM((3, 8, 1, NBLK), I32),
        pltpu.VMEM((OWN_ROWS, W), I32), pltpu.VMEM((GROUP_ROWS, W), I32),
        pltpu.SMEM((OWN_ROWS, W), I32), pltpu.SMEM((GROUP_ROWS, W), I32),
        pltpu.VMEM((4, 1, NBLK), I32), pltpu.VMEM((4, 1, NBLK), I32),
        pltpu.VMEM((NBLK, W, W), BF16), pltpu.VMEM((NBLK, W, W), BF16), pltpu.VMEM((TILES, CH, W), BF16),
    ]
    scratch += [
        pltpu.SemaphoreType.DMA((n, 2, PARTS, 9)), pltpu.SemaphoreType.DMA((n, 2, PARTS, 10)),
        pltpu.SemaphoreType.DMA((n, PARTS, 5, 6)), pltpu.SemaphoreType.DMA((n, PARTS, 5, 6)),
        pltpu.SemaphoreType.DMA((n, PARTS, 5, 4)), pltpu.SemaphoreType.DMA((n, PARTS, 5, 4)),
        pltpu.SemaphoreType.DMA((5, 8)), pltpu.SemaphoreType.DMA((5, 8)), pltpu.SemaphoreType.DMA((3,)),
    ]
    vmem = pl.BlockSpec(memory_space=pltpu.VMEM)
    return pl.pallas_call(
        functools.partial(body, cap, halves, unrolled, plan),
        out_shape=(
            result, result, jax.ShapeDtypeStruct((1,), I32)
        ),
        in_specs=[pl.BlockSpec(memory_space=pltpu.SMEM)] * 2 + [vmem] * 6 + [pl.BlockSpec(memory_space=pl.ANY)],
        out_specs=(vmem, vmem, pl.BlockSpec(memory_space=pltpu.SMEM)),
        scratch_shapes=scratch,
        compiler_params=pltpu.CompilerParams(
            collective_id=which, has_side_effects=True, vmem_limit_bytes=66 * 1024 * 1024 - 2200000
        ),
    )(src, valid, goal, source, ice, ocean, mask, rate, weights)


def on_device(ice_state, ocean_state, ice_rate, block_weights, block_route, block_tiles, block_valid, ice_mask):
    cats, fields, cells = ice_state.shape
    chans = cats * fields
    source = block_tiles[:, 0]
    goal = (block_route[:, 0] * TILES + block_tiles[:, 1]).reshape(1, NBLK)
    rate = ice_rate.reshape(chans, 1)
    mask = ice_mask.astype(F32)[None, :]
    given = source, block_valid, goal, source.reshape(1, NBLK), ice_state, ocean_state, mask, rate, block_weights
    ice, flux, over = couple(FEW, 0, HALVES, True, PLAN, *given)

    def again(ice, flux, *given):
        ice, flux, unused = couple(MOST, 1, (ROWS,), False, (), *given)
        return ice, flux

    def keep(ice, flux, *given):
        return ice, flux

    ice, flux = lax.cond(over[0] > 0, again, keep, ice, flux, *given)
    return ice, flux


def solution(mesh):
    placed = (
        P(None, None, ("ice", "ocn")),
        P(None, None, ("ice", "ocn")),
        P(),
        P(("ice", "ocn"), None, None),
        P(("ice", "ocn"), None),
        P(("ice", "ocn"), None),
        P(("ice", "ocn")),
        P(("ice", "ocn")),
    )
    return jax.shard_map(
        on_device,
        mesh=mesh,
        in_specs=placed,
        out_specs=(P(None, None, ("ice", "ocn")), P(None, None, ("ice", "ocn"))),
        check_vma=False,
    )
```
